128 devices in a mesh: depth: 4 (over x_lo, core), lat: 32 (over z, x_hi, y).
Axes of the slice: x: 4 (x_hi: 2, x_lo: 2; x = x_hi * 2 + x_lo), y: 4, z: 4, core: 2. Of those that a mesh axis runs over, the one named last changes fastest.
Arguments:
- source: float32 [4, 2, 320, 128, 512], P(None, None, 'depth', 'lat'), may hold values from -6 to 6
- line_inverse: float32 [4, 2, 80, 80], P('depth'), may hold values from -0.6 to 1.6, as said below
- plane_count: int32 [4], P('depth'), may hold values from 48 to 80
- classes: int32 [320, 128, 512], P('depth', 'lat'), may hold values from 0 to 15
- table_re: float32 [16], replicated, may hold values from -2 to 2
- table_im: float32 [16], replicated, may hold values from 0.5 to 2
Outputs:
- field: float32 [4, 2, 320, 128, 512], P(None, None, 'depth', 'lat')
The draws below stay inside these ranges and needn't reach their ends.
Inputs may be any that keep to these rules, and one draw needn't show every extreme that they name: `line_inverse`: a dense complex matrix for each layer whose real diagonal is about 0.8.
All inputs are finite; a program needn't handle non-finite values.
Results may differ from the reference program's by a relative error of at most 0.0001.
Values sent between devices are 32-bit elements; how exact they have to be, the bound alone decides.
A program may use at most 128 MiB of HBM per device.

```python
import jax
import jax.numpy as jnp
from jax import lax

SHOTS = 4
PLANES = 80
CLASSES = 16
NY = 512
NX = 128
NZ = 320
N_DEPTH = 4


def draw_line_inverse(key, part):
    shape = (N_DEPTH, 2, PLANES, PLANES)
    spread = jnp.clip(0.15 * jax.random.normal(jax.random.fold_in(key, 7), shape, jnp.float32), -0.6, 0.6)
    unit = jnp.eye(PLANES, dtype=jnp.float32)
    return spread.at[:, 0].add(unit[None] * (1.0 - jnp.abs(spread[:, 0])) * 0.8)


def touch_ends(drawn, stream_key, smallest, high):
    index_at = [jax.random.randint(jax.random.fold_in(stream_key, axis), (), 0, length) for axis, length in enumerate(drawn.shape)]
    main_axis = drawn.shape.index(max(drawn.shape))
    neighbour = index_at[:main_axis] + [(index_at[main_axis] + 1) % drawn.shape[main_axis]] + index_at[main_axis + 1:]
    return drawn.at[tuple(index_at)].set(smallest).at[tuple(neighbour)].set(high)


def levels(rng, extent, shards, least, largest):
    level, own = 1.0, jax.random.fold_in(rng, 6)
    for axis_at, parts in shards:
        heights = jnp.exp(jax.random.uniform(jax.random.fold_in(own, axis_at), (parts,), jnp.float32, least / len(shards), largest / len(shards)))
        level = level * jnp.repeat(heights, extent[axis_at] // parts).reshape([-1 if axis == axis_at else 1 for axis in range(len(extent))])
    return level


def normal_values(key, extent, scale, reach, shards=(), kind=jnp.bfloat16):
    values = jax.random.normal(key, extent, jnp.float32) * scale
    if len(shards) > 0:
        values = levels(key, extent, shards, -0.22, 0.18) * values
    return jnp.clip(values, min=-reach, max=reach).astype(kind)


def setup_inputs(seed: int = 0) -> dict:
    key_list = jax.random.split(jax.random.key(seed), 7)
    source = normal_values(key_list[0], (SHOTS, 2, NZ, NX, NY), 1.0, 6.0, ((2, 4), (3, 32)), jnp.float32)
    line_inverse = draw_line_inverse(jax.random.fold_in(key_list[6], 71), 0)
    plane_count = touch_ends(jax.random.randint(key_list[2], (N_DEPTH,), PLANES * 3 // 5, PLANES + 1), jax.random.fold_in(key_list[2], 1), PLANES * 3 // 5, PLANES).astype(jnp.int32)
    classes = touch_ends(jax.random.randint(key_list[3], (NZ, NX, NY), 0, CLASSES), jax.random.fold_in(key_list[3], 1), 0, CLASSES - 1).astype(jnp.int32)
    table_re = jnp.clip(jax.random.uniform(key_list[4], (CLASSES,), jnp.float32, -2.0, 2.0), -2.0, 2.0)
    table_im = jnp.clip(jax.random.uniform(key_list[5], (CLASSES,), jnp.float32, 0.5, 2.0), 0.5, 2.0)
    return dict(source=source, line_inverse=line_inverse, plane_count=plane_count, classes=classes, table_re=table_re, table_im=table_im)


CORRECTION = 0.1


def lateral(padded):
    width = [(0, 0)] * (padded.ndim - 1) + [(2, 2)]
    grid = jnp.pad(padded, width)
    center = grid[..., 2:-2, 2:-2]
    along_x = -(grid[..., :-4, 2:-2] + grid[..., 4:, 2:-2]) / 12.0 + (grid[..., 1:-3, 2:-2] + grid[..., 3:-1, 2:-2]) * (4.0 / 3.0)
    along_y = -(grid[..., 2:-2, :-4] + grid[..., 2:-2, 4:]) / 12.0 + (grid[..., 2:-2, 1:-3] + grid[..., 2:-2, 3:-1]) * (4.0 / 3.0)
    return along_x + along_y - 5.0 * center


def lookup(classes, table_re, table_im):
    kappa_re = jnp.zeros(classes.shape, jnp.float32)
    kappa_im = jnp.zeros(classes.shape, jnp.float32)
    for index in range(CLASSES):
        hit = classes == index
        kappa_re = jnp.where(hit, table_re[index], kappa_re)
        kappa_im = jnp.where(hit, table_im[index], kappa_im)
    return kappa_re, kappa_im


def plane_product(matrix, field):
    real = jnp.einsum("pq,sqxy->spxy", matrix[0], field[:, 0], precision=lax.Precision.HIGHEST) - jnp.einsum("pq,sqxy->spxy", matrix[1], field[:, 1], precision=lax.Precision.HIGHEST)
    imag = jnp.einsum("pq,sqxy->spxy", matrix[0], field[:, 1], precision=lax.Precision.HIGHEST) + jnp.einsum("pq,sqxy->spxy", matrix[1], field[:, 0], precision=lax.Precision.HIGHEST)
    return jnp.stack([real, imag], axis=1)


def layer_map(source, matrix, count, classes, table_re, table_im, inbound_down, inbound_up):
    half = SHOTS // 2
    index = jnp.arange(PLANES, dtype=jnp.int32)
    live = (index < count).astype(jnp.float32)[:, None, None]
    first = (index == 0).astype(jnp.float32)[:, None, None]
    last = (index == count - 1).astype(jnp.float32)[:, None, None]
    inject = jnp.concatenate([first * inbound_down[:, :, None], last * inbound_up[:, :, None]], axis=0)
    solved = plane_product(matrix, live * (source + inject))
    padded = jnp.pad(solved, [(0, 0), (0, 0), (0, 0), (2, 2), (0, 0)])
    kappa_re, kappa_im = lookup(classes, table_re, table_im)
    mixed = jnp.stack([kappa_re * solved[:, 0] - kappa_im * solved[:, 1], kappa_re * solved[:, 1] + kappa_im * solved[:, 0]], axis=1)
    result = live * (solved + CORRECTION * (lateral(padded) + mixed))
    trace_down = jnp.sum(result[:half] * last, axis=2)
    trace_up = result[half:, :, 0]
    return result, trace_down, trace_up


def reference(source, line_inverse, plane_count, classes, table_re, table_im):
    half = SHOTS // 2
    zeros = jnp.zeros((half, 2, source.shape[3], source.shape[4]), jnp.float32)

    def run(layer, inbound_down, inbound_up):
        low = layer * PLANES
        return layer_map(source[:, :, low:low + PLANES], line_inverse[layer], plane_count[layer], classes[low:low + PLANES], table_re, table_im, inbound_down, inbound_up)

    downs = []
    carried = zeros
    for layer in range(N_DEPTH):
        downs.append(carried)
        carried = run(layer, carried, zeros)[1]
    ups = [zeros] * N_DEPTH
    carried = zeros
    for layer in reversed(range(N_DEPTH)):
        ups[layer] = carried
        carried = run(layer, zeros, carried)[2]
    pieces = [run(layer, downs[layer], ups[layer])[0] for layer in range(N_DEPTH)]
    return jnp.concatenate(pieces, axis=2)
```

```python
import functools

import jax
import jax.numpy as jnp
from jax import lax
from jax.experimental import pallas as pl
from jax.experimental.pallas import tpu as pltpu
from jax.sharding import PartitionSpec as P

MESH = pl.DeviceIdType.MESH
CLASSES = 16
CORRECTION = 0.1
NEAR = 4.0 / 3.0
FAR = -1.0 / 12.0
BLOCK = 16
EXTRA = 16
PIECES_FIRST = 2
PIECES_BASE_OUTER = 1
PIECES_BASE_INNER = 2
PIECES_TRACE = 1


def along_y(x):
    size = x.shape[1]
    lane = lax.broadcasted_iota(jnp.int32, x.shape, 1)
    near = jnp.where(lane >= 1, pltpu.roll(x, 1, 1), 0.0) + jnp.where(
        lane < size - 1, pltpu.roll(x, size - 1, 1), 0.0
    )
    far = jnp.where(lane >= 2, pltpu.roll(x, 2, 1), 0.0) + jnp.where(
        lane < size - 2, pltpu.roll(x, size - 2, 1), 0.0
    )
    return NEAR * near + FAR * far


def field_kernel(
    source, matrix, count, classes, table_re, table_im, field,
    held, cells, solved, halo, kappa, plane, base, inbound, outbound, spread, column, coeff, weights,
    load_sem, cell_sem, bulk_send, bulk_recv, base_send, base_recv, trace_send, trace_recv,
):
    shots, rows, _, planes, width = held.shape
    half = shots // 2
    pieces = shots * 4
    d = lax.axis_index("depth")
    l = lax.axis_index("lat")
    layers = lax.axis_size("depth")
    tiles = lax.axis_size("lat")
    has_prev = l > 0
    has_next = l < tiles - 1
    inner = (d > 0) & (d < layers - 1)
    last = count[0] - 1

    def load(s, r):
        return pltpu.make_async_copy(source.at[s, :, :, r, :], held.at[s, r], load_sem.at[s, r])

    def load_cells(r):
        return pltpu.make_async_copy(classes.at[:, r, :], cells.at[r], cell_sem.at[r])

    for r in (0, 3, 1, 2):
        load(0, r).start()
    for s in range(1, shots):
        for r in range(rows):
            load(s, r).start()
    for r in range(rows):
        load_cells(r).start()

    base[...] = jnp.zeros_like(base)
    inbound[...] = jnp.zeros_like(inbound)

    barrier = pltpu.get_barrier_semaphore()
    expected = 0
    for by_d in (-1, 0, 1):
        for by_l in (-1, 0, 1):
            if by_d == 0 and by_l == 0:
                continue
            there = (d + by_d >= 0) & (d + by_d < layers) & (l + by_l >= 0) & (l + by_l < tiles)
            expected = expected + jnp.where(there, 1, 0)

            @pl.when(there)
            def _():
                pl.semaphore_signal(barrier, inc=1, device_id=(d + by_d, l + by_l), device_id_type=MESH)

    at_row = lax.broadcasted_iota(jnp.int32, (planes, planes), 0)
    at_column = lax.broadcasted_iota(jnp.int32, (planes, planes), 1)
    live = (at_row <= last) & (at_column <= last)
    real = jnp.where(live, matrix[0, 0], 0.0)
    imag = jnp.where(live, matrix[0, 1], 0.0)
    end_re = jnp.sum(jnp.where(at_row == last, real, 0.0), axis=0, keepdims=True)
    end_im = jnp.sum(jnp.where(at_row == last, imag, 0.0), axis=0, keepdims=True)
    whole = jnp.concatenate(
        [
            jnp.concatenate([real, -imag], axis=1),
            jnp.concatenate([imag, real], axis=1),
            jnp.concatenate(
                [
                    jnp.concatenate([end_re, -end_im], axis=1),
                    jnp.concatenate([end_im, end_re], axis=1),
                    jnp.concatenate([real[:1], -imag[:1]], axis=1),
                    jnp.concatenate([imag[:1], real[:1]], axis=1),
                    jnp.zeros((EXTRA - 4, 2 * planes), jnp.float32),
                ],
                axis=0,
            ),
        ],
        axis=0,
    )
    high = whole.astype(jnp.bfloat16)
    low = (whole - high.astype(jnp.float32)).astype(jnp.bfloat16)
    tall = 2 * planes + EXTRA
    weights[:tall] = high
    weights[tall:] = low
    for side, pick in ((0, at_column == 0), (1, at_column == last)):
        for part, values in ((0, real), (1, imag)):
            picked = jnp.sum(jnp.where(pick, values, 0.0), axis=1, keepdims=True)
            column[side, part] = jnp.broadcast_to(picked, (planes, 128))
    for part, values in ((0, real), (1, imag)):
        for side, pick in ((0, (at_row == last) & (at_column == 0)), (1, (at_row == 0) & (at_column == last))):
            picked = jnp.sum(jnp.sum(jnp.where(pick, values, 0.0), axis=1, keepdims=True), axis=0, keepdims=True)
            coeff[side, part] = jnp.broadcast_to(picked, (half, 128))

    def solve(s, r):
        load(s, r).wait()
        values = held[s, r].reshape(2 * planes, width)
        upper = values.astype(jnp.bfloat16)
        lower = (values - upper.astype(jnp.float32)).astype(jnp.bfloat16)
        first = jnp.dot(weights[...], upper, preferred_element_type=jnp.float32)
        second = jnp.dot(weights[:tall], lower, preferred_element_type=jnp.float32)
        total = first[:tall] + first[tall:] + second
        solved[s, r] = total[: 2 * planes].reshape(2, planes, width)
        side = s // half
        for part in range(2):
            row = jnp.where(
                side == 0,
                total[2 * planes + part : 2 * planes + part + 1],
                total[2 * planes + 2 + part : 2 * planes + 3 + part],
            )
            base[side, part, r + 2, pl.ds(s % half, 1), :] = row

    def piece(k, to_next):
        s, a, part = k // 4, (k % 4) // 2, k % 2
        if to_next:
            return pltpu.make_async_remote_copy(
                src_ref=solved.at[s, 3 - a, part],
                dst_ref=halo.at[s, 1 - a, part],
                send_sem=bulk_send.at[1, k],
                recv_sem=bulk_recv.at[1, k],
                device_id=(d, l + 1),
                device_id_type=MESH,
            )
        return pltpu.make_async_remote_copy(
            src_ref=solved.at[s, a, part],
            dst_ref=halo.at[s, 2 + a, part],
            send_sem=bulk_send.at[0, k],
            recv_sem=bulk_recv.at[0, k],
            device_id=(d, l - 1),
            device_id_type=MESH,
        )

    def send_pieces(start, stop):
        for to_next, there in ((False, has_prev), (True, has_next)):

            @pl.when(there)
            def _():
                def step(k, carry):
                    piece(k, to_next).start()
                    return carry

                lax.fori_loop(start, stop, step, 0)

    solve(0, 0)
    solve(0, 3)
    pl.semaphore_wait(barrier, expected)
    send_pieces(0, PIECES_FIRST)
    solve(0, 1)
    solve(0, 2)

    def solve_shot(s, carry):
        for r in range(rows):
            solve(s, r)
        return carry

    lax.fori_loop(1, shots, solve_shot, 0)

    def base_copy(to_next):
        if to_next:
            return pltpu.make_async_remote_copy(
                src_ref=base.at[:, :, pl.ds(4, 2)],
                dst_ref=base.at[:, :, pl.ds(0, 2)],
                send_sem=base_send.at[1],
                recv_sem=base_recv.at[1],
                device_id=(d, l + 1),
                device_id_type=MESH,
            )
        return pltpu.make_async_remote_copy(
            src_ref=base.at[:, :, pl.ds(2, 2)],
            dst_ref=base.at[:, :, pl.ds(6, 2)],
            send_sem=base_send.at[0],
            recv_sem=base_recv.at[0],
            device_id=(d, l - 1),
            device_id_type=MESH,
        )

    for to_next, there in ((False, has_prev), (True, has_next)):

        @pl.when(there)
        def _():
            base_copy(to_next).start()

    @pl.when(inner)
    def _():
        send_pieces(PIECES_FIRST, PIECES_FIRST + PIECES_BASE_INNER)

    @pl.when(jnp.logical_not(inner))
    def _():
        send_pieces(PIECES_FIRST, PIECES_FIRST + PIECES_BASE_OUTER)

    for r in range(rows):
        load_cells(r).wait()

        def look_up(i, carry):
            at = pl.ds(pl.multiple_of(i * BLOCK, BLOCK), BLOCK)
            kinds = cells[r, at, :]
            re = jnp.full(kinds.shape, table_re[0], jnp.float32)
            im = jnp.full(kinds.shape, table_im[0], jnp.float32)
            for kind in range(1, CLASSES):
                hit = kinds == kind
                re = jnp.where(hit, table_re[kind], re)
                im = jnp.where(hit, table_im[kind], im)
            kappa[r, 0, at, :] = re
            kappa[r, 1, at, :] = im
            bottom = lax.broadcasted_iota(jnp.int32, kinds.shape, 0) + i * BLOCK == last
            return (carry[0] + jnp.where(bottom, re, 0.0), carry[1] + jnp.where(bottom, im, 0.0))

        zeros = jnp.zeros((BLOCK, width), jnp.float32)
        sums = lax.fori_loop(0, planes // BLOCK, look_up, (zeros, zeros))
        for part in range(2):
            plane[0, part, r] = jnp.broadcast_to(jnp.sum(sums[part], axis=0, keepdims=True), (half, width))
            plane[1, part, r] = jnp.broadcast_to(kappa[r, part, pl.ds(0, 1), :], (half, width))

    @pl.when(has_prev)
    def _():
        base_copy(True).wait_recv()

    @pl.when(has_next)
    def _():
        base_copy(False).wait_recv()

    def lateral(values, r):
        at = r + 2
        return (
            NEAR * (values[at - 1] + values[at + 1])
            + FAR * (values[at - 2] + values[at + 2])
            + along_y(values[at])
            - 5.0 * values[at]
        )

    def trace_copies(side):
        to = d + 1 - 2 * side
        return (
            (
                True,
                True,
                lambda: pltpu.make_async_remote_copy(
                    src_ref=outbound.at[side],
                    dst_ref=inbound.at[side, :, pl.ds(2, 4)],
                    send_sem=trace_send.at[side, 0],
                    recv_sem=trace_recv.at[side, 0],
                    device_id=(to, l),
                    device_id_type=MESH,
                ),
            ),
            (
                has_prev,
                has_next,
                lambda: pltpu.make_async_remote_copy(
                    src_ref=outbound.at[side, :, pl.ds(0, 2)],
                    dst_ref=inbound.at[side, :, pl.ds(6, 2)],
                    send_sem=trace_send.at[side, 1],
                    recv_sem=trace_recv.at[side, 1],
                    device_id=(to, l - 1),
                    device_id_type=MESH,
                ),
            ),
            (
                has_next,
                has_prev,
                lambda: pltpu.make_async_remote_copy(
                    src_ref=outbound.at[side, :, pl.ds(2, 2)],
                    dst_ref=inbound.at[side, :, pl.ds(0, 2)],
                    send_sem=trace_send.at[side, 2],
                    recv_sem=trace_recv.at[side, 2],
                    device_id=(to, l + 1),
                    device_id_type=MESH,
                ),
            ),
        )

    def under(there, act):
        if there is True:
            act()
        else:
            pl.when(there)(act)

    def emit(side):
        factor = [
            jnp.concatenate([coeff[side, part]] * (width // 128), axis=1) for part in range(2)
        ]
        planar = ([], [])
        for row in range(rows + 4):
            t_re, t_im = inbound[side, 0, row], inbound[side, 1, row]
            planar[0].append(base[side, 0, row] + factor[0] * t_re - factor[1] * t_im)
            planar[1].append(base[side, 1, row] + factor[0] * t_im + factor[1] * t_re)
        for r in range(rows):
            re, im = planar[0][r + 2], planar[1][r + 2]
            k_re, k_im = plane[side, 0, r], plane[side, 1, r]
            outbound[side, 0, r] = re + CORRECTION * (lateral(planar[0], r) + k_re * re - k_im * im)
            outbound[side, 1, r] = im + CORRECTION * (lateral(planar[1], r) + k_re * im + k_im * re)
        for goes, _, copy in trace_copies(side):
            under(goes, lambda: copy().start())

    def take(side):
        for _, comes, copy in trace_copies(side):
            under(comes, lambda: copy().wait_recv())

    side_one = jnp.where(d >= layers // 2, 1, 0)
    side_two = 1 - side_one

    @pl.when(inner)
    def _():
        take(side_one)

    emit(side_one)
    sent_inner = PIECES_FIRST + PIECES_BASE_INNER

    @pl.when(inner)
    def _():
        send_pieces(sent_inner, sent_inner + PIECES_TRACE)

    @pl.when(jnp.logical_not(inner))
    def _():
        send_pieces(PIECES_FIRST + PIECES_BASE_OUTER, pieces)

    take(side_two)

    @pl.when(inner)
    def _():
        emit(side_two)
        send_pieces(sent_inner + PIECES_TRACE, pieces)

    for side in range(2):
        for part in range(2):
            values = [inbound[side, part, row] for row in range(rows + 4)]
            for r in range(rows):
                spread[side, part, r] = values[r + 2] + CORRECTION * lateral(values, r)

    def own_rows(s, carry):
        side, shot = s // half, s % half
        for r in range(rows):
            t = [inbound[side, part, r + 2, pl.ds(shot, 1), :] for part in range(2)]
            e = [spread[side, part, r, pl.ds(shot, 1), :] for part in range(2)]

            def block(i, inside):
                at = pl.ds(pl.multiple_of(i * BLOCK, BLOCK), BLOCK)
                g_re, g_im = (
                    jnp.concatenate([column[side, part, at, :]] * (width // 128), axis=1) for part in range(2)
                )
                linear, values = [], []
                for part in range(2):
                    v = solved[s, r, part, at, :]
                    near = [solved[s, q, part, at, :] for q in (r - 1, r + 1) if 0 <= q < rows]
                    far = [solved[s, q, part, at, :] for q in (r - 2, r + 2) if 0 <= q < rows]
                    total = along_y(v) - 5.0 * v + NEAR * sum(near[1:], near[0]) + FAR * sum(far[1:], far[0])
                    linear.append(v + CORRECTION * total)
                    values.append(v)
                v_re = values[0] + g_re * t[0] - g_im * t[1]
                v_im = values[1] + g_re * t[1] + g_im * t[0]
                k_re, k_im = kappa[r, 0, at, :], kappa[r, 1, at, :]
                field[s, r, 0, at, :] = (
                    linear[0] + g_re * e[0] - g_im * e[1] + CORRECTION * (k_re * v_re - k_im * v_im)
                )
                field[s, r, 1, at, :] = (
                    linear[1] + g_re * e[1] + g_im * e[0] + CORRECTION * (k_re * v_im + k_im * v_re)
                )
                return inside

            lax.fori_loop(0, planes // BLOCK, block, 0)
        return carry

    lax.fori_loop(0, shots, own_rows, 0)

    def add_rows(s, part, q, to_rows):
        def block(i, inside):
            at = pl.ds(pl.multiple_of(i * BLOCK, BLOCK), BLOCK)
            v = halo[s, q, part, at, :]
            for r, weight in to_rows:
                field[s, r, part, at, :] = field[s, r, part, at, :] + (CORRECTION * weight) * v
            return inside

        lax.fori_loop(0, planes // BLOCK, block, 0)

    def add_shot(s, carry):
        for a in range(2):
            for part in range(2):
                k = s * 4 + a * 2 + part

                @pl.when(has_next)
                def _():
                    piece(k, False).wait_recv()
                    add_rows(s, part, 2 + a, ((3, NEAR), (2, FAR)) if a == 0 else ((3, FAR),))

                @pl.when(has_prev)
                def _():
                    piece(k, True).wait_recv()
                    add_rows(s, part, 1 - a, ((0, NEAR), (1, FAR)) if a == 0 else ((0, FAR),))
        return carry

    lax.fori_loop(0, shots, add_shot, 0)

    for to_next, there in ((False, has_prev), (True, has_next)):

        @pl.when(there)
        def _():
            base_copy(to_next).wait_send()

            def step(k, carry):
                piece(k, to_next).wait_send()
                return carry

            lax.fori_loop(0, pieces, step, 0)

    for goes, _, copy in trace_copies(side_one):
        under(goes, lambda: copy().wait_send())

    @pl.when(inner)
    def _():
        for goes, _, copy in trace_copies(side_two):
            under(goes, lambda: copy().wait_send())


def write_kernel(field, out, sem):
    shots, rows = field.shape[:2]

    def copy(s, r):
        return pltpu.make_async_copy(field.at[s, r], out.at[s, :, :, r, :], sem.at[s, r])

    for s in range(shots):
        for r in range(rows):
            copy(s, r).start()
    for s in range(shots):
        for r in range(rows):
            copy(s, r).wait()


def on_device(source, line_inverse, plane_count, classes, table_re, table_im):
    shots, parts, planes, rows, width = source.shape
    half = shots // 2
    by_rows = (shots, rows, parts, planes, width)
    any_space = pl.BlockSpec(memory_space=pl.ANY)
    vmem = pl.BlockSpec(memory_space=pltpu.VMEM)
    smem = pl.BlockSpec(memory_space=pltpu.SMEM)
    tall = 2 * planes + EXTRA
    pieces = shots * 4
    dma = pltpu.SemaphoreType.DMA
    field = pl.pallas_call(
        field_kernel,
        out_shape=jax.ShapeDtypeStruct(by_rows, jnp.float32),
        in_specs=[any_space, vmem, smem, any_space, smem, smem],
        out_specs=vmem,
        scratch_shapes=[
            pltpu.VMEM(by_rows, jnp.float32),
            pltpu.VMEM((rows, planes, width), jnp.int32),
            pltpu.VMEM(by_rows, jnp.float32),
            pltpu.VMEM((shots, 4, parts, planes, width), jnp.float32),
            pltpu.VMEM((rows, parts, planes, width), jnp.float32),
            pltpu.VMEM((2, parts, rows, half, width), jnp.float32),
            pltpu.VMEM((2, parts, rows + 4, half, width), jnp.float32),
            pltpu.VMEM((2, parts, rows + 4, half, width), jnp.float32),
            pltpu.VMEM((2, parts, rows, half, width), jnp.float32),
            pltpu.VMEM((2, parts, rows, half, width), jnp.float32),
            pltpu.VMEM((2, parts, planes, 128), jnp.float32),
            pltpu.VMEM((2, parts, half, 128), jnp.float32),
            pltpu.VMEM((2 * tall, 2 * planes), jnp.bfloat16),
            dma((shots, rows)),
            dma((rows,)),
            dma((2, pieces)),
            dma((2, pieces)),
            dma((2,)),
            dma((2,)),
            dma((2, 3)),
            dma((2, 3)),
        ],
        compiler_params=pltpu.CompilerParams(
            collective_id=0, has_side_effects=True, vmem_limit_bytes=56 * 2**20
        ),
    )(source, line_inverse, plane_count, classes, table_re, table_im)
    return pl.pallas_call(
        write_kernel,
        out_shape=jax.ShapeDtypeStruct(source.shape, jnp.float32),
        in_specs=[vmem],
        out_specs=any_space,
        scratch_shapes=[dma((shots, rows))],
        compiler_params=pltpu.CompilerParams(vmem_limit_bytes=8 * 2**20),
    )(field)


def solution(mesh):
    in_specs = (
        P(None, None, "depth", "lat", None),
        P("depth", None, None, None),
        P("depth"),
        P("depth", "lat", None),
        P(),
        P(),
    )
    out_specs = P(None, None, "depth", "lat", None)
    return jax.shard_map(
        on_device, mesh=mesh, in_specs=in_specs, out_specs=out_specs, check_vma=False
    )
```

```python
import functools

import jax
import jax.numpy as jnp
from jax import lax
from jax.experimental import pallas as pl
from jax.experimental.pallas import tpu as pltpu
from jax.sharding import PartitionSpec as P

MESH = pl.DeviceIdType.MESH
CLASSES = 16
CORRECTION = 0.1
NEAR = 4.0 / 3.0
FAR = -1.0 / 12.0
BLOCK = 16
EXTRA = 16
PIECES_FIRST = 2
PIECES_BASE_OUTER = 1
PIECES_BASE_INNER = 2
PIECES_TRACE = 1


def along_y(x):
    size = x.shape[1]
    lane = lax.broadcasted_iota(jnp.int32, x.shape, 1)
    near = jnp.where(lane >= 1, pltpu.roll(x, 1, 1), 0.0) + jnp.where(
        lane < size - 1, pltpu.roll(x, size - 1, 1), 0.0
    )
    far = jnp.where(lane >= 2, pltpu.roll(x, 2, 1), 0.0) + jnp.where(
        lane < size - 2, pltpu.roll(x, size - 2, 1), 0.0
    )
    return NEAR * near + FAR * far


def field_kernel(
    count, source, matrix_from, classes, table_re_from, table_im_from, field,
    matrix, table_re, table_im,
    held, cells, solved, halo, kappa, plane, base, inbound, outbound, spread, column, coeff, weights,
    small_sem, load_sem, cell_sem, bulk_send, bulk_recv, base_send, base_recv, trace_send, trace_recv,
):
    shots, rows, _, planes, width = held.shape
    half = shots // 2
    pieces = shots * 4
    d = lax.axis_index("depth")
    l = lax.axis_index("lat")
    layers = lax.axis_size("depth")
    tiles = lax.axis_size("lat")
    has_prev = l > 0
    has_next = l < tiles - 1
    inner = (d > 0) & (d < layers - 1)

    def load(s, r):
        return pltpu.make_async_copy(source.at[s, :, :, r, :], held.at[s, r], load_sem.at[s, r])

    def load_cells(r):
        return pltpu.make_async_copy(classes.at[:, r, :], cells.at[r], cell_sem.at[r])

    small = [
        pltpu.make_async_copy(here, there, small_sem.at[i])
        for i, (here, there) in enumerate(
            ((matrix_from.at[0], matrix), (table_re_from, table_re), (table_im_from, table_im))
        )
    ]
    small[0].start()
    for r in (0, 3, 1, 2):
        load(0, r).start()
    small[1].start()
    small[2].start()
    for s in range(1, shots):
        for r in range(rows):
            load(s, r).start()
    for r in range(rows):
        load_cells(r).start()

    base[...] = jnp.zeros_like(base)
    inbound[...] = jnp.zeros_like(inbound)

    barrier = pltpu.get_barrier_semaphore()
    expected = 0
    for by_d in (-1, 0, 1):
        for by_l in (-1, 0, 1):
            if by_d == 0 and by_l == 0:
                continue
            there = (d + by_d >= 0) & (d + by_d < layers) & (l + by_l >= 0) & (l + by_l < tiles)
            expected = expected + jnp.where(there, 1, 0)

            @pl.when(there)
            def _():
                pl.semaphore_signal(barrier, inc=1, device_id=(d + by_d, l + by_l), device_id_type=MESH)

    small[0].wait()
    last = count[0] - 1
    at_row = lax.broadcasted_iota(jnp.int32, (planes, planes), 0)
    at_column = lax.broadcasted_iota(jnp.int32, (planes, planes), 1)
    live = (at_row <= last) & (at_column <= last)
    real = jnp.where(live, matrix[0], 0.0)
    imag = jnp.where(live, matrix[1], 0.0)
    end_re = jnp.sum(jnp.where(at_row == last, real, 0.0), axis=0, keepdims=True)
    end_im = jnp.sum(jnp.where(at_row == last, imag, 0.0), axis=0, keepdims=True)
    whole = jnp.concatenate(
        [
            jnp.concatenate([real, -imag], axis=1),
            jnp.concatenate([imag, real], axis=1),
            jnp.concatenate(
                [
                    jnp.concatenate([end_re, -end_im], axis=1),
                    jnp.concatenate([end_im, end_re], axis=1),
                    jnp.concatenate([real[:1], -imag[:1]], axis=1),
                    jnp.concatenate([imag[:1], real[:1]], axis=1),
                    jnp.zeros((EXTRA - 4, 2 * planes), jnp.float32),
                ],
                axis=0,
            ),
        ],
        axis=0,
    )
    high = whole.astype(jnp.bfloat16)
    low = (whole - high.astype(jnp.float32)).astype(jnp.bfloat16)
    tall = 2 * planes + EXTRA
    weights[:tall] = high
    weights[tall:] = low
    for side, pick in ((0, at_column == 0), (1, at_column == last)):
        for part, values in ((0, real), (1, imag)):
            picked = jnp.sum(jnp.where(pick, values, 0.0), axis=1, keepdims=True)
            column[side, part] = jnp.broadcast_to(picked, (planes, 128))
    for part, values in ((0, real), (1, imag)):
        for side, pick in ((0, (at_row == last) & (at_column == 0)), (1, (at_row == 0) & (at_column == last))):
            picked = jnp.sum(jnp.sum(jnp.where(pick, values, 0.0), axis=1, keepdims=True), axis=0, keepdims=True)
            coeff[side, part] = jnp.broadcast_to(picked, (half, 128))

    def solve(s, r):
        load(s, r).wait()
        values = held[s, r].reshape(2 * planes, width)
        upper = values.astype(jnp.bfloat16)
        lower = (values - upper.astype(jnp.float32)).astype(jnp.bfloat16)
        first = jnp.dot(weights[...], upper, preferred_element_type=jnp.float32)
        second = jnp.dot(weights[:tall], lower, preferred_element_type=jnp.float32)
        total = first[:tall] + first[tall:] + second
        solved[s, r] = total[: 2 * planes].reshape(2, planes, width)
        side = s // half
        for part in range(2):
            row = jnp.where(
                side == 0,
                total[2 * planes + part : 2 * planes + part + 1],
                total[2 * planes + 2 + part : 2 * planes + 3 + part],
            )
            base[side, part, r + 2, pl.ds(s % half, 1), :] = row

    def piece(k, to_next):
        s, a, part = k // 4, (k % 4) // 2, k % 2
        if to_next:
            return pltpu.make_async_remote_copy(
                src_ref=solved.at[s, 3 - a, part],
                dst_ref=halo.at[s, 1 - a, part],
                send_sem=bulk_send.at[1, k],
                recv_sem=bulk_recv.at[1, k],
                device_id=(d, l + 1),
                device_id_type=MESH,
            )
        return pltpu.make_async_remote_copy(
            src_ref=solved.at[s, a, part],
            dst_ref=halo.at[s, 2 + a, part],
            send_sem=bulk_send.at[0, k],
            recv_sem=bulk_recv.at[0, k],
            device_id=(d, l - 1),
            device_id_type=MESH,
        )

    def send_pieces(start, stop):
        for to_next, there in ((False, has_prev), (True, has_next)):

            @pl.when(there)
            def _():
                def step(k, carry):
                    piece(k, to_next).start()
                    return carry

                lax.fori_loop(start, stop, step, 0)

    solve(0, 0)
    solve(0, 3)
    pl.semaphore_wait(barrier, expected)
    send_pieces(0, PIECES_FIRST)
    solve(0, 1)
    solve(0, 2)

    def solve_shot(s, carry):
        for r in range(rows):
            solve(s, r)
        return carry

    lax.fori_loop(1, shots, solve_shot, 0)

    def base_copy(to_next):
        if to_next:
            return pltpu.make_async_remote_copy(
                src_ref=base.at[:, :, pl.ds(4, 2)],
                dst_ref=base.at[:, :, pl.ds(0, 2)],
                send_sem=base_send.at[1],
                recv_sem=base_recv.at[1],
                device_id=(d, l + 1),
                device_id_type=MESH,
            )
        return pltpu.make_async_remote_copy(
            src_ref=base.at[:, :, pl.ds(2, 2)],
            dst_ref=base.at[:, :, pl.ds(6, 2)],
            send_sem=base_send.at[0],
            recv_sem=base_recv.at[0],
            device_id=(d, l - 1),
            device_id_type=MESH,
        )

    for to_next, there in ((False, has_prev), (True, has_next)):

        @pl.when(there)
        def _():
            base_copy(to_next).start()

    @pl.when(inner)
    def _():
        send_pieces(PIECES_FIRST, PIECES_FIRST + PIECES_BASE_INNER)

    @pl.when(jnp.logical_not(inner))
    def _():
        send_pieces(PIECES_FIRST, PIECES_FIRST + PIECES_BASE_OUTER)

    small[1].wait()
    small[2].wait()
    for r in range(rows):
        load_cells(r).wait()

        def look_up(i, carry):
            at = pl.ds(pl.multiple_of(i * BLOCK, BLOCK), BLOCK)
            kinds = cells[r, at, :]
            re = jnp.full(kinds.shape, table_re[0], jnp.float32)
            im = jnp.full(kinds.shape, table_im[0], jnp.float32)
            for kind in range(1, CLASSES):
                hit = kinds == kind
                re = jnp.where(hit, table_re[kind], re)
                im = jnp.where(hit, table_im[kind], im)
            kappa[r, 0, at, :] = re
            kappa[r, 1, at, :] = im
            bottom = lax.broadcasted_iota(jnp.int32, kinds.shape, 0) + i * BLOCK == last
            return (carry[0] + jnp.where(bottom, re, 0.0), carry[1] + jnp.where(bottom, im, 0.0))

        zeros = jnp.zeros((BLOCK, width), jnp.float32)
        sums = lax.fori_loop(0, planes // BLOCK, look_up, (zeros, zeros))
        for part in range(2):
            plane[0, part, r] = jnp.broadcast_to(jnp.sum(sums[part], axis=0, keepdims=True), (half, width))
            plane[1, part, r] = jnp.broadcast_to(kappa[r, part, pl.ds(0, 1), :], (half, width))

    @pl.when(has_prev)
    def _():
        base_copy(True).wait_recv()

    @pl.when(has_next)
    def _():
        base_copy(False).wait_recv()

    def lateral(values, r):
        at = r + 2
        return (
            NEAR * (values[at - 1] + values[at + 1])
            + FAR * (values[at - 2] + values[at + 2])
            + along_y(values[at])
            - 5.0 * values[at]
        )

    def trace_copies(side):
        to = d + 1 - 2 * side
        return (
            (
                True,
                True,
                lambda: pltpu.make_async_remote_copy(
                    src_ref=outbound.at[side],
                    dst_ref=inbound.at[side, :, pl.ds(2, 4)],
                    send_sem=trace_send.at[side, 0],
                    recv_sem=trace_recv.at[side, 0],
                    device_id=(to, l),
                    device_id_type=MESH,
                ),
            ),
            (
                has_prev,
                has_next,
                lambda: pltpu.make_async_remote_copy(
                    src_ref=outbound.at[side, :, pl.ds(0, 2)],
                    dst_ref=inbound.at[side, :, pl.ds(6, 2)],
                    send_sem=trace_send.at[side, 1],
                    recv_sem=trace_recv.at[side, 1],
                    device_id=(to, l - 1),
                    device_id_type=MESH,
                ),
            ),
            (
                has_next,
                has_prev,
                lambda: pltpu.make_async_remote_copy(
                    src_ref=outbound.at[side, :, pl.ds(2, 2)],
                    dst_ref=inbound.at[side, :, pl.ds(0, 2)],
                    send_sem=trace_send.at[side, 2],
                    recv_sem=trace_recv.at[side, 2],
                    device_id=(to, l + 1),
                    device_id_type=MESH,
                ),
            ),
        )

    def under(there, act):
        if there is True:
            act()
        else:
            pl.when(there)(act)

    def emit(side):
        factor = [
            jnp.concatenate([coeff[side, part]] * (width // 128), axis=1) for part in range(2)
        ]
        planar = ([], [])
        for row in range(rows + 4):
            t_re, t_im = inbound[side, 0, row], inbound[side, 1, row]
            planar[0].append(base[side, 0, row] + factor[0] * t_re - factor[1] * t_im)
            planar[1].append(base[side, 1, row] + factor[0] * t_im + factor[1] * t_re)
        for r in range(rows):
            re, im = planar[0][r + 2], planar[1][r + 2]
            k_re, k_im = plane[side, 0, r], plane[side, 1, r]
            outbound[side, 0, r] = re + CORRECTION * (lateral(planar[0], r) + k_re * re - k_im * im)
            outbound[side, 1, r] = im + CORRECTION * (lateral(planar[1], r) + k_re * im + k_im * re)
        for goes, _, copy in trace_copies(side):
            under(goes, lambda: copy().start())

    def take(side):
        for _, comes, copy in trace_copies(side):
            under(comes, lambda: copy().wait_recv())

    side_one = jnp.where(d >= layers // 2, 1, 0)
    side_two = 1 - side_one

    @pl.when(inner)
    def _():
        take(side_one)

    emit(side_one)
    sent_inner = PIECES_FIRST + PIECES_BASE_INNER

    @pl.when(inner)
    def _():
        send_pieces(sent_inner, sent_inner + PIECES_TRACE)

    @pl.when(jnp.logical_not(inner))
    def _():
        send_pieces(PIECES_FIRST + PIECES_BASE_OUTER, pieces)

    take(side_two)

    @pl.when(inner)
    def _():
        emit(side_two)
        send_pieces(sent_inner + PIECES_TRACE, pieces)

    for side in range(2):
        for part in range(2):
            values = [inbound[side, part, row] for row in range(rows + 4)]
            for r in range(rows):
                spread[side, part, r] = values[r + 2] + CORRECTION * lateral(values, r)

    def own_rows(s, carry):
        side, shot = s // half, s % half
        for r in range(rows):
            t = [inbound[side, part, r + 2, pl.ds(shot, 1), :] for part in range(2)]
            e = [spread[side, part, r, pl.ds(shot, 1), :] for part in range(2)]

            def block(i, inside):
                at = pl.ds(pl.multiple_of(i * BLOCK, BLOCK), BLOCK)
                g_re, g_im = (
                    jnp.concatenate([column[side, part, at, :]] * (width // 128), axis=1) for part in range(2)
                )
                linear, values = [], []
                for part in range(2):
                    v = solved[s, r, part, at, :]
                    near = [solved[s, q, part, at, :] for q in (r - 1, r + 1) if 0 <= q < rows]
                    far = [solved[s, q, part, at, :] for q in (r - 2, r + 2) if 0 <= q < rows]
                    total = along_y(v) - 5.0 * v + NEAR * sum(near[1:], near[0]) + FAR * sum(far[1:], far[0])
                    linear.append(v + CORRECTION * total)
                    values.append(v)
                v_re = values[0] + g_re * t[0] - g_im * t[1]
                v_im = values[1] + g_re * t[1] + g_im * t[0]
                k_re, k_im = kappa[r, 0, at, :], kappa[r, 1, at, :]
                field[s, r, 0, at, :] = (
                    linear[0] + g_re * e[0] - g_im * e[1] + CORRECTION * (k_re * v_re - k_im * v_im)
                )
                field[s, r, 1, at, :] = (
                    linear[1] + g_re * e[1] + g_im * e[0] + CORRECTION * (k_re * v_im + k_im * v_re)
                )
                return inside

            lax.fori_loop(0, planes // BLOCK, block, 0)
        return carry

    lax.fori_loop(0, shots, own_rows, 0)

    def add_rows(s, part, q, to_rows):
        def block(i, inside):
            at = pl.ds(pl.multiple_of(i * BLOCK, BLOCK), BLOCK)
            v = halo[s, q, part, at, :]
            for r, weight in to_rows:
                field[s, r, part, at, :] = field[s, r, part, at, :] + (CORRECTION * weight) * v
            return inside

        lax.fori_loop(0, planes // BLOCK, block, 0)

    def add_shot(s, carry):
        for a in range(2):
            for part in range(2):
                k = s * 4 + a * 2 + part

                @pl.when(has_next)
                def _():
                    piece(k, False).wait_recv()
                    add_rows(s, part, 2 + a, ((3, NEAR), (2, FAR)) if a == 0 else ((3, FAR),))

                @pl.when(has_prev)
                def _():
                    piece(k, True).wait_recv()
                    add_rows(s, part, 1 - a, ((0, NEAR), (1, FAR)) if a == 0 else ((0, FAR),))
        return carry

    lax.fori_loop(0, shots, add_shot, 0)

    for to_next, there in ((False, has_prev), (True, has_next)):

        @pl.when(there)
        def _():
            base_copy(to_next).wait_send()

            def step(k, carry):
                piece(k, to_next).wait_send()
                return carry

            lax.fori_loop(0, pieces, step, 0)

    for goes, _, copy in trace_copies(side_one):
        under(goes, lambda: copy().wait_send())

    @pl.when(inner)
    def _():
        for goes, _, copy in trace_copies(side_two):
            under(goes, lambda: copy().wait_send())


def write_kernel(field, out, sem):
    shots, rows = field.shape[:2]

    def copy(s, r):
        return pltpu.make_async_copy(field.at[s, r], out.at[s, :, :, r, :], sem.at[s, r])

    for s in range(shots):
        for r in range(rows):
            copy(s, r).start()
    for s in range(shots):
        for r in range(rows):
            copy(s, r).wait()


def on_device(source, line_inverse, plane_count, classes, table_re, table_im):
    shots, parts, planes, rows, width = source.shape
    half = shots // 2
    by_rows = (shots, rows, parts, planes, width)
    any_space = pl.BlockSpec(memory_space=pl.ANY)
    hbm = pl.BlockSpec(memory_space=pltpu.HBM)
    vmem = pl.BlockSpec(memory_space=pltpu.VMEM)
    tall = 2 * planes + EXTRA
    pieces = shots * 4
    dma = pltpu.SemaphoreType.DMA
    operands = (source, line_inverse, classes, table_re, table_im)
    field = pl.pallas_call(
        field_kernel,
        out_shape=jax.ShapeDtypeStruct(by_rows, jnp.float32),
        in_specs=[pl.BlockSpec(memory_space=pltpu.SMEM)] + [hbm] * len(operands),
        out_specs=vmem,
        scratch_shapes=[
            pltpu.VMEM((parts, planes, planes), jnp.float32),
            pltpu.SMEM((CLASSES,), jnp.float32),
            pltpu.SMEM((CLASSES,), jnp.float32),
            pltpu.VMEM(by_rows, jnp.float32),
            pltpu.VMEM((rows, planes, width), jnp.int32),
            pltpu.VMEM(by_rows, jnp.float32),
            pltpu.VMEM((shots, 4, parts, planes, width), jnp.float32),
            pltpu.VMEM((rows, parts, planes, width), jnp.float32),
            pltpu.VMEM((2, parts, rows, half, width), jnp.float32),
            pltpu.VMEM((2, parts, rows + 4, half, width), jnp.float32),
            pltpu.VMEM((2, parts, rows + 4, half, width), jnp.float32),
            pltpu.VMEM((2, parts, rows, half, width), jnp.float32),
            pltpu.VMEM((2, parts, rows, half, width), jnp.float32),
            pltpu.VMEM((2, parts, planes, 128), jnp.float32),
            pltpu.VMEM((2, parts, half, 128), jnp.float32),
            pltpu.VMEM((2 * tall, 2 * planes), jnp.bfloat16),
            dma((3,)),
            dma((shots, rows)),
            dma((rows,)),
            dma((2, pieces)),
            dma((2, pieces)),
            dma((2,)),
            dma((2,)),
            dma((2, 3)),
            dma((2, 3)),
        ],
        compiler_params=pltpu.CompilerParams(
            collective_id=0, has_side_effects=True, vmem_limit_bytes=40 * 2**20
        ),
    )(plane_count, *(pltpu.with_memory_space_constraint(x, pltpu.HBM) for x in operands))
    return pl.pallas_call(
        write_kernel,
        out_shape=jax.ShapeDtypeStruct(source.shape, jnp.float32),
        in_specs=[vmem],
        out_specs=any_space,
        scratch_shapes=[dma((shots, rows))],
        compiler_params=pltpu.CompilerParams(vmem_limit_bytes=8 * 2**20),
    )(field)


def solution(mesh):
    in_specs = (
        P(None, None, "depth", "lat", None),
        P("depth", None, None, None),
        P("depth"),
        P("depth", "lat", None),
        P(),
        P(),
    )
    out_specs = P(None, None, "depth", "lat", None)
    return jax.shard_map(
        on_device, mesh=mesh, in_specs=in_specs, out_specs=out_specs, check_vma=False
    )
```

```python
import functools

import jax
import jax.numpy as jnp
from jax import lax
from jax.experimental import pallas as pl
from jax.experimental.pallas import tpu as pltpu
from jax.sharding import PartitionSpec as P

MESH = pl.DeviceIdType.MESH
CLASSES = 16
CORRECTION = 0.1
NEAR = 4.0 / 3.0
FAR = -1.0 / 12.0
BLOCK = 16
EXTRA = 16
PIECES_FIRST = 2
PIECES_SOLVE = 3
PIECES_BASE_OUTER = 2
PIECES_BASE_INNER = 4
PIECES_TRACE = 3


def along_y(x):
    size = x.shape[1]
    lane = lax.broadcasted_iota(jnp.int32, x.shape, 1)
    near = jnp.where(lane >= 1, pltpu.roll(x, 1, 1), 0.0) + jnp.where(
        lane < size - 1, pltpu.roll(x, size - 1, 1), 0.0
    )
    far = jnp.where(lane >= 2, pltpu.roll(x, 2, 1), 0.0) + jnp.where(
        lane < size - 2, pltpu.roll(x, size - 2, 1), 0.0
    )
    return NEAR * near + FAR * far


def field_kernel(
    count, source, matrix_from, classes, table_re_from, table_im_from, field,
    matrix, table_re, table_im,
    held, cells, solved, halo, kappa, plane, base, inbound, outbound, spread, column, coeff, weights,
    small_sem, load_sem, cell_sem, bulk_send, bulk_recv, base_send, base_recv, trace_send, trace_recv,
    ready_sem,
):
    shots, rows, _, planes, width = held.shape
    half = shots // 2
    pieces = shots * 4
    d = lax.axis_index("depth")
    l = lax.axis_index("lat")
    layers = lax.axis_size("depth")
    tiles = lax.axis_size("lat")
    has_prev = l > 0
    has_next = l < tiles - 1
    has_above = d > 0
    has_below = d < layers - 1
    inner = has_above & has_below
    side_one = jnp.where(d >= layers // 2, 1, 0)
    side_two = 1 - side_one

    def load(s, r):
        return pltpu.make_async_copy(source.at[s, :, :, r, :], held.at[s, r], load_sem.at[s, r])

    def load_cells(r):
        return pltpu.make_async_copy(classes.at[:, r, :], cells.at[r], cell_sem.at[r])

    small = [
        pltpu.make_async_copy(here, there, small_sem.at[i])
        for i, (here, there) in enumerate(
            ((matrix_from.at[0], matrix), (table_re_from, table_re), (table_im_from, table_im))
        )
    ]
    barrier = pltpu.get_barrier_semaphore()
    beside = ((has_prev, 0, -1), (has_next, 0, 1), (has_above, -1, 0), (has_below, 1, 0))
    for there, by_d, by_l in beside:

        @pl.when(there)
        def _():
            pl.semaphore_signal(barrier, inc=1, device_id=(d + by_d, l + by_l), device_id_type=MESH)

    expected = sum(jnp.where(there, 1, 0) for there, _, _ in beside)

    small[0].start()
    for r in (0, 3, 1, 2):
        load(0, r).start()
    small[1].start()
    small[2].start()
    for s in range(1, shots):
        for r in range(rows):
            load(s, r).start()
    for r in range(rows):
        load_cells(r).start()

    for there, at in ((has_prev, pl.ds(0, 2)), (has_next, pl.ds(6, 2))):

        @pl.when(jnp.logical_not(there))
        def _():
            base[:, :, at] = jnp.zeros((2, 2, 2, half, width), jnp.float32)
            inbound[:, :, at] = jnp.zeros((2, 2, 2, half, width), jnp.float32)

    for there, side in ((has_above, 0), (has_below, 1)):

        @pl.when(jnp.logical_not(there))
        def _():
            inbound[side] = jnp.zeros(inbound.shape[1:], jnp.float32)

    small[0].wait()
    last = count[0] - 1
    at_row = lax.broadcasted_iota(jnp.int32, (planes, planes), 0)
    at_column = lax.broadcasted_iota(jnp.int32, (planes, planes), 1)
    live = (at_row <= last) & (at_column <= last)
    real = jnp.where(live, matrix[0], 0.0)
    imag = jnp.where(live, matrix[1], 0.0)
    end_re = jnp.sum(jnp.where(at_row == last, real, 0.0), axis=0, keepdims=True)
    end_im = jnp.sum(jnp.where(at_row == last, imag, 0.0), axis=0, keepdims=True)
    whole = jnp.concatenate(
        [
            jnp.concatenate([real, -imag], axis=1),
            jnp.concatenate([imag, real], axis=1),
            jnp.concatenate(
                [
                    jnp.concatenate([end_re, -end_im], axis=1),
                    jnp.concatenate([end_im, end_re], axis=1),
                    jnp.concatenate([real[:1], -imag[:1]], axis=1),
                    jnp.concatenate([imag[:1], real[:1]], axis=1),
                    jnp.zeros((EXTRA - 4, 2 * planes), jnp.float32),
                ],
                axis=0,
            ),
        ],
        axis=0,
    )
    high = whole.astype(jnp.bfloat16)
    low = (whole - high.astype(jnp.float32)).astype(jnp.bfloat16)
    tall = 2 * planes + EXTRA
    weights[:tall] = high
    weights[tall:] = low
    for side, pick in ((0, at_column == 0), (1, at_column == last)):
        for part, values in ((0, real), (1, imag)):
            picked = jnp.sum(jnp.where(pick, values, 0.0), axis=1, keepdims=True)
            column[side, part] = jnp.broadcast_to(picked, (planes, 128))
    for part, values in ((0, real), (1, imag)):
        for side, pick in ((0, (at_row == last) & (at_column == 0)), (1, (at_row == 0) & (at_column == last))):
            picked = jnp.sum(jnp.sum(jnp.where(pick, values, 0.0), axis=1, keepdims=True), axis=0, keepdims=True)
            coeff[side, part] = jnp.broadcast_to(picked, (half, 128))

    def solve(s, r):
        load(s, r).wait()
        values = held[s, r].reshape(2 * planes, width)
        upper = values.astype(jnp.bfloat16)
        lower = (values - upper.astype(jnp.float32)).astype(jnp.bfloat16)
        first = jnp.dot(weights[...], upper, preferred_element_type=jnp.float32)
        second = jnp.dot(weights[:tall], lower, preferred_element_type=jnp.float32)
        total = first[:tall] + first[tall:] + second
        solved[s, r] = total[: 2 * planes].reshape(2, planes, width)
        side = s // half
        for part in range(2):
            row = jnp.where(
                side == 0,
                total[2 * planes + part : 2 * planes + part + 1],
                total[2 * planes + 2 + part : 2 * planes + 3 + part],
            )
            base[side, part, r + 2, pl.ds(s % half, 1), :] = row

    def piece(k, to_next):
        s, a, part = k // 4, (k % 4) // 2, k % 2
        if to_next:
            return pltpu.make_async_remote_copy(
                src_ref=solved.at[s, 3 - a, part],
                dst_ref=halo.at[s, 1 - a, part],
                send_sem=bulk_send.at[1, k],
                recv_sem=bulk_recv.at[1, k],
                device_id=(d, l + 1),
                device_id_type=MESH,
            )
        return pltpu.make_async_remote_copy(
            src_ref=solved.at[s, a, part],
            dst_ref=halo.at[s, 2 + a, part],
            send_sem=bulk_send.at[0, k],
            recv_sem=bulk_recv.at[0, k],
            device_id=(d, l - 1),
            device_id_type=MESH,
        )

    def send_pieces(start, stop):
        for to_next, there in ((False, has_prev), (True, has_next)):

            @pl.when(there)
            def _():
                def step(k, carry):
                    piece(k, to_next).start()
                    return carry

                lax.fori_loop(start, stop, step, 0)

    solve(0, 0)
    solve(0, 3)
    pl.semaphore_wait(barrier, expected)
    send_pieces(0, PIECES_FIRST)
    for there, by_d in ((has_above, -1), (has_below, 1)):

        @pl.when(there)
        def _():
            pl.semaphore_signal(ready_sem, inc=1, device_id=(d + by_d, l), device_id_type=MESH)

    solve(0, 1)
    solve(0, 2)
    send_pieces(PIECES_FIRST, PIECES_SOLVE)

    def solve_shot(s, carry):
        for r in range(rows):
            solve(s, r)
        return carry

    lax.fori_loop(1, shots, solve_shot, 0)

    def base_copy(side, to_next):
        source_at, target_at = (4, 0) if to_next else (2, 6)
        return pltpu.make_async_remote_copy(
            src_ref=base.at[side, :, pl.ds(source_at, 2)],
            dst_ref=base.at[side, :, pl.ds(target_at, 2)],
            send_sem=base_send.at[int(to_next), side],
            recv_sem=base_recv.at[int(to_next), side],
            device_id=(d, l + 1 if to_next else l - 1),
            device_id_type=MESH,
        )

    base_copies = tuple(
        (needed, to_next, side)
        for needed, side in ((True, side_one), (inner, side_two))
        for to_next in (False, True)
    )

    def both(needed, there):
        return there if needed is True else needed & there

    for needed, to_next, side in base_copies:

        @pl.when(both(needed, has_next if to_next else has_prev))
        def _():
            base_copy(side, to_next).start()

    @pl.when(inner)
    def _():
        send_pieces(PIECES_SOLVE, PIECES_SOLVE + PIECES_BASE_INNER)

    @pl.when(jnp.logical_not(inner))
    def _():
        send_pieces(PIECES_SOLVE, PIECES_SOLVE + PIECES_BASE_OUTER)

    small[1].wait()
    small[2].wait()
    for r in range(rows):
        load_cells(r).wait()

        def look_up(i, carry):
            at = pl.ds(pl.multiple_of(i * BLOCK, BLOCK), BLOCK)
            kinds = cells[r, at, :]
            re = jnp.full(kinds.shape, table_re[0], jnp.float32)
            im = jnp.full(kinds.shape, table_im[0], jnp.float32)
            for kind in range(1, CLASSES):
                hit = kinds == kind
                re = jnp.where(hit, table_re[kind], re)
                im = jnp.where(hit, table_im[kind], im)
            kappa[r, 0, at, :] = re
            kappa[r, 1, at, :] = im
            bottom = lax.broadcasted_iota(jnp.int32, kinds.shape, 0) + i * BLOCK == last
            return (carry[0] + jnp.where(bottom, re, 0.0), carry[1] + jnp.where(bottom, im, 0.0))

        zeros = jnp.zeros((BLOCK, width), jnp.float32)
        sums = lax.fori_loop(0, planes // BLOCK, look_up, (zeros, zeros))
        for part in range(2):
            plane[0, part, r] = jnp.broadcast_to(jnp.sum(sums[part], axis=0, keepdims=True), (half, width))
            plane[1, part, r] = jnp.broadcast_to(kappa[r, part, pl.ds(0, 1), :], (half, width))

    for needed, to_next, side in base_copies:

        @pl.when(both(needed, has_prev if to_next else has_next))
        def _():
            base_copy(side, to_next).wait_recv()

    pl.semaphore_wait(ready_sem, jnp.where(has_above, 1, 0) + jnp.where(has_below, 1, 0))

    def lateral(values, r):
        at = r + 2
        return (
            NEAR * (values[at - 1] + values[at + 1])
            + FAR * (values[at - 2] + values[at + 2])
            + along_y(values[at])
            - 5.0 * values[at]
        )

    def trace_copies(side):
        to = d + 1 - 2 * side
        return (
            (
                True,
                True,
                lambda: pltpu.make_async_remote_copy(
                    src_ref=outbound.at[side],
                    dst_ref=inbound.at[side, :, pl.ds(2, 4)],
                    send_sem=trace_send.at[side, 0],
                    recv_sem=trace_recv.at[side, 0],
                    device_id=(to, l),
                    device_id_type=MESH,
                ),
            ),
            (
                has_prev,
                has_next,
                lambda: pltpu.make_async_remote_copy(
                    src_ref=outbound.at[side, :, pl.ds(0, 2)],
                    dst_ref=inbound.at[side, :, pl.ds(6, 2)],
                    send_sem=trace_send.at[side, 1],
                    recv_sem=trace_recv.at[side, 1],
                    device_id=(to, l - 1),
                    device_id_type=MESH,
                ),
            ),
            (
                has_next,
                has_prev,
                lambda: pltpu.make_async_remote_copy(
                    src_ref=outbound.at[side, :, pl.ds(2, 2)],
                    dst_ref=inbound.at[side, :, pl.ds(0, 2)],
                    send_sem=trace_send.at[side, 2],
                    recv_sem=trace_recv.at[side, 2],
                    device_id=(to, l + 1),
                    device_id_type=MESH,
                ),
            ),
        )

    def under(there, act):
        if there is True:
            act()
        else:
            pl.when(there)(act)

    def emit(side):
        factor = [
            jnp.concatenate([coeff[side, part]] * (width // 128), axis=1) for part in range(2)
        ]
        planar = ([], [])
        for row in range(rows + 4):
            t_re, t_im = inbound[side, 0, row], inbound[side, 1, row]
            planar[0].append(base[side, 0, row] + factor[0] * t_re - factor[1] * t_im)
            planar[1].append(base[side, 1, row] + factor[0] * t_im + factor[1] * t_re)
        for r in range(rows):
            re, im = planar[0][r + 2], planar[1][r + 2]
            k_re, k_im = plane[side, 0, r], plane[side, 1, r]
            outbound[side, 0, r] = re + CORRECTION * (lateral(planar[0], r) + k_re * re - k_im * im)
            outbound[side, 1, r] = im + CORRECTION * (lateral(planar[1], r) + k_re * im + k_im * re)
        for goes, _, copy in trace_copies(side):
            under(goes, lambda: copy().start())

    def take(side):
        for _, comes, copy in trace_copies(side):
            under(comes, lambda: copy().wait_recv())

    @pl.when(inner)
    def _():
        take(side_one)

    emit(side_one)
    sent_inner = PIECES_SOLVE + PIECES_BASE_INNER

    @pl.when(inner)
    def _():
        send_pieces(sent_inner, sent_inner + PIECES_TRACE)

    @pl.when(jnp.logical_not(inner))
    def _():
        send_pieces(PIECES_SOLVE + PIECES_BASE_OUTER, pieces)

    take(side_two)

    @pl.when(inner)
    def _():
        emit(side_two)
        send_pieces(sent_inner + PIECES_TRACE, pieces)

    for side in range(2):
        for part in range(2):
            values = [inbound[side, part, row] for row in range(rows + 4)]
            for r in range(rows):
                spread[side, part, r] = values[r + 2] + CORRECTION * lateral(values, r)

    def own_rows(s, carry):
        side, shot = s // half, s % half
        for r in range(rows):
            t = [inbound[side, part, r + 2, pl.ds(shot, 1), :] for part in range(2)]
            e = [spread[side, part, r, pl.ds(shot, 1), :] for part in range(2)]

            def block(i, inside):
                at = pl.ds(pl.multiple_of(i * BLOCK, BLOCK), BLOCK)
                g_re, g_im = (
                    jnp.concatenate([column[side, part, at, :]] * (width // 128), axis=1) for part in range(2)
                )
                linear, values = [], []
                for part in range(2):
                    v = solved[s, r, part, at, :]
                    near = [solved[s, q, part, at, :] for q in (r - 1, r + 1) if 0 <= q < rows]
                    far = [solved[s, q, part, at, :] for q in (r - 2, r + 2) if 0 <= q < rows]
                    total = along_y(v) - 5.0 * v + NEAR * sum(near[1:], near[0]) + FAR * sum(far[1:], far[0])
                    linear.append(v + CORRECTION * total)
                    values.append(v)
                v_re = values[0] + g_re * t[0] - g_im * t[1]
                v_im = values[1] + g_re * t[1] + g_im * t[0]
                k_re, k_im = kappa[r, 0, at, :], kappa[r, 1, at, :]
                field[s, r, 0, at, :] = (
                    linear[0] + g_re * e[0] - g_im * e[1] + CORRECTION * (k_re * v_re - k_im * v_im)
                )
                field[s, r, 1, at, :] = (
                    linear[1] + g_re * e[1] + g_im * e[0] + CORRECTION * (k_re * v_im + k_im * v_re)
                )
                return inside

            lax.fori_loop(0, planes // BLOCK, block, 0)
        return carry

    lax.fori_loop(0, shots, own_rows, 0)

    def add_rows(s, part, q, to_rows):
        for first in range(0, planes, BLOCK):
            at = pl.ds(first, BLOCK)
            v = halo[s, q, part, at, :]
            for r, weight in to_rows:
                field[s, r, part, at, :] = field[s, r, part, at, :] + (CORRECTION * weight) * v

    for needed, to_next, side in base_copies:

        @pl.when(both(needed, has_next if to_next else has_prev))
        def _():
            base_copy(side, to_next).wait_send()

    for goes, _, copy in trace_copies(side_one):
        under(goes, lambda: copy().wait_send())

    @pl.when(inner)
    def _():
        for goes, _, copy in trace_copies(side_two):
            under(goes, lambda: copy().wait_send())

    def add_shot(s, carry):
        for a in range(2):
            for part in range(2):
                k = s * 4 + a * 2 + part

                @pl.when(has_next)
                def _():
                    piece(k, False).wait_recv()
                    piece(k, True).wait_send()
                    add_rows(s, part, 2 + a, ((3, NEAR), (2, FAR)) if a == 0 else ((3, FAR),))

                @pl.when(has_prev)
                def _():
                    piece(k, True).wait_recv()
                    piece(k, False).wait_send()
                    add_rows(s, part, 1 - a, ((0, NEAR), (1, FAR)) if a == 0 else ((0, FAR),))
        return carry

    lax.fori_loop(0, shots, add_shot, 0)


def write_kernel(field, out, sem):
    shots, rows = field.shape[:2]

    def copy(s, r):
        return pltpu.make_async_copy(field.at[s, r], out.at[s, :, :, r, :], sem.at[s, r])

    for s in range(shots):
        for r in range(rows):
            copy(s, r).start()
    for s in range(shots):
        for r in range(rows):
            copy(s, r).wait()


def on_device(source, line_inverse, plane_count, classes, table_re, table_im):
    shots, parts, planes, rows, width = source.shape
    half = shots // 2
    by_rows = (shots, rows, parts, planes, width)
    any_space = pl.BlockSpec(memory_space=pl.ANY)
    hbm = pl.BlockSpec(memory_space=pltpu.HBM)
    vmem = pl.BlockSpec(memory_space=pltpu.VMEM)
    tall = 2 * planes + EXTRA
    pieces = shots * 4
    dma = pltpu.SemaphoreType.DMA
    operands = (source, line_inverse, classes, table_re, table_im)
    field = pl.pallas_call(
        field_kernel,
        out_shape=jax.ShapeDtypeStruct(by_rows, jnp.float32),
        in_specs=[pl.BlockSpec(memory_space=pltpu.SMEM)] + [hbm] * len(operands),
        out_specs=vmem,
        scratch_shapes=[
            pltpu.VMEM((parts, planes, planes), jnp.float32),
            pltpu.SMEM((CLASSES,), jnp.float32),
            pltpu.SMEM((CLASSES,), jnp.float32),
            pltpu.VMEM(by_rows, jnp.float32),
            pltpu.VMEM((rows, planes, width), jnp.int32),
            pltpu.VMEM(by_rows, jnp.float32),
            pltpu.VMEM((shots, 4, parts, planes, width), jnp.float32),
            pltpu.VMEM((rows, parts, planes, width), jnp.float32),
            pltpu.VMEM((2, parts, rows, half, width), jnp.float32),
            pltpu.VMEM((2, parts, rows + 4, half, width), jnp.float32),
            pltpu.VMEM((2, parts, rows + 4, half, width), jnp.float32),
            pltpu.VMEM((2, parts, rows, half, width), jnp.float32),
            pltpu.VMEM((2, parts, rows, half, width), jnp.float32),
            pltpu.VMEM((2, parts, planes, 128), jnp.float32),
            pltpu.VMEM((2, parts, half, 128), jnp.float32),
            pltpu.VMEM((2 * tall, 2 * planes), jnp.bfloat16),
            dma((3,)),
            dma((shots, rows)),
            dma((rows,)),
            dma((2, pieces)),
            dma((2, pieces)),
            dma((2, 2)),
            dma((2, 2)),
            dma((2, 3)),
            dma((2, 3)),
            pltpu.SemaphoreType.REGULAR,
        ],
        compiler_params=pltpu.CompilerParams(
            collective_id=0, has_side_effects=True, vmem_limit_bytes=40 * 2**20
        ),
    )(plane_count, *(pltpu.with_memory_space_constraint(x, pltpu.HBM) for x in operands))
    return pl.pallas_call(
        write_kernel,
        out_shape=jax.ShapeDtypeStruct(source.shape, jnp.float32),
        in_specs=[vmem],
        out_specs=any_space,
        scratch_shapes=[dma((shots, rows))],
        compiler_params=pltpu.CompilerParams(vmem_limit_bytes=8 * 2**20),
    )(field)


def solution(mesh):
    in_specs = (
        P(None, None, "depth", "lat", None),
        P("depth", None, None, None),
        P("depth"),
        P("depth", "lat", None),
        P(),
        P(),
    )
    out_specs = P(None, None, "depth", "lat", None)
    return jax.shard_map(
        on_device, mesh=mesh, in_specs=in_specs, out_specs=out_specs, check_vma=False
    )
```

```python
import functools

import jax
import jax.numpy as jnp
from jax import lax
from jax.experimental import pallas as pl
from jax.experimental.pallas import tpu as pltpu
from jax.sharding import PartitionSpec as P

MESH = pl.DeviceIdType.MESH
CLASSES = 16
CORRECTION = 0.1
NEAR = 4.0 / 3.0
FAR = -1.0 / 12.0
BLOCK = 16
EXTRA = 16
RING = 4
RELAY = 40
HELD_BACK = 4
PIECES_FIRST = 2
PIECES_SOLVE = 3
PIECES_BASE_OUTER = 2
PIECES_BASE_INNER = 4
PIECES_TRACE = 3


def along_y(x):
    size = x.shape[1]
    lane = lax.broadcasted_iota(jnp.int32, x.shape, 1)
    near = jnp.where(lane >= 1, pltpu.roll(x, 1, 1), 0.0) + jnp.where(
        lane < size - 1, pltpu.roll(x, size - 1, 1), 0.0
    )
    far = jnp.where(lane >= 2, pltpu.roll(x, 2, 1), 0.0) + jnp.where(
        lane < size - 2, pltpu.roll(x, size - 2, 1), 0.0
    )
    return NEAR * near + FAR * far


def field_kernel(
    count, source, matrix_from, classes, table_re_from, table_im_from, field,
    matrix, table_re, table_im,
    held, cells, solved, halo, kappa, plane, base, inbound, outbound, spread, column, coeff, weights,
    small_sem, load_sem, cell_sem, bulk_send, bulk_recv, base_send, base_recv, trace_send, trace_recv,
    ready_sem, near_sem, relay_send, relay_recv, passed,
):
    shots, rows, _, planes, width = held.shape
    half = shots // 2
    pieces = shots * 4
    d = lax.axis_index("depth")
    l = lax.axis_index("lat")
    layers = lax.axis_size("depth")
    tiles = lax.axis_size("lat")
    has_prev = l > 0
    has_next = l < tiles - 1
    has_above = d > 0
    has_below = d < layers - 1
    inner = has_above & has_below
    seam_prev = has_prev & (l % RING == 0)
    seam_next = has_next & (l % RING == RING - 1)
    seam = seam_prev | seam_next
    at_pair = l % (2 * RING)

    def seam_at(tile):
        at = tile % RING
        return ((tile > 0) & (at == 0)) | ((tile < tiles - 1) & (at == RING - 1))

    side_one = jnp.where(d >= layers // 2, 1, 0)
    side_two = 1 - side_one

    def load(s, r):
        return pltpu.make_async_copy(source.at[s, :, :, r, :], held.at[s, r], load_sem.at[s, r])

    def load_cells(r):
        return pltpu.make_async_copy(classes.at[:, r, :], cells.at[r], cell_sem.at[r])

    small = [
        pltpu.make_async_copy(here, there, small_sem.at[i])
        for i, (here, there) in enumerate(
            ((matrix_from.at[0], matrix), (table_re_from, table_re), (table_im_from, table_im))
        )
    ]
    barrier = pltpu.get_barrier_semaphore()
    for there, by_d, by_l in (
        (has_prev & (seam | jnp.logical_not(seam_at(l - 1))), 0, -1),
        (has_next & (seam | jnp.logical_not(seam_at(l + 1))), 0, 1),
        (has_above & jnp.logical_not(seam), -1, 0),
        (has_below & jnp.logical_not(seam), 1, 0),
        ((at_pair == 5) & (l > 5), 0, -7),
        ((at_pair == 2) & (l + 6 < tiles), 0, 7),
    ):

        @pl.when(there)
        def _():
            pl.semaphore_signal(barrier, inc=1, device_id=(d + by_d, l + by_l), device_id_type=MESH)

    layers_beside = jnp.where(has_above, 1, 0) + jnp.where(has_below, 1, 0)
    tiles_beside = jnp.where(has_prev, 1, 0) + jnp.where(has_next, 1, 0)
    tiles_beyond = jnp.where(((at_pair == 6) & (l + 2 < tiles)) | ((at_pair == 1) & (l > 1)), 1, 0)

    small[0].start()
    for r in (0, 3, 1, 2):
        load(0, r).start()
    small[1].start()
    small[2].start()
    for s in range(1, shots):
        for r in range(rows):
            load(s, r).start()
    for r in range(rows):
        load_cells(r).start()

    for there, at in ((has_prev, pl.ds(0, 2)), (has_next, pl.ds(6, 2))):

        @pl.when(jnp.logical_not(there))
        def _():
            base[:, :, at] = jnp.zeros((2, 2, 2, half, width), jnp.float32)
            inbound[:, :, at] = jnp.zeros((2, 2, 2, half, width), jnp.float32)

    for there, side in ((has_above, 0), (has_below, 1)):

        @pl.when(jnp.logical_not(there))
        def _():
            inbound[side] = jnp.zeros(inbound.shape[1:], jnp.float32)

    small[0].wait()
    last = count[0] - 1
    at_row = lax.broadcasted_iota(jnp.int32, (planes, planes), 0)
    at_column = lax.broadcasted_iota(jnp.int32, (planes, planes), 1)
    live = (at_row <= last) & (at_column <= last)
    real = jnp.where(live, matrix[0], 0.0)
    imag = jnp.where(live, matrix[1], 0.0)
    end_re = jnp.sum(jnp.where(at_row == last, real, 0.0), axis=0, keepdims=True)
    end_im = jnp.sum(jnp.where(at_row == last, imag, 0.0), axis=0, keepdims=True)
    whole = jnp.concatenate(
        [
            jnp.concatenate([real, -imag], axis=1),
            jnp.concatenate([imag, real], axis=1),
            jnp.concatenate(
                [
                    jnp.concatenate([end_re, -end_im], axis=1),
                    jnp.concatenate([end_im, end_re], axis=1),
                    jnp.concatenate([real[:1], -imag[:1]], axis=1),
                    jnp.concatenate([imag[:1], real[:1]], axis=1),
                    jnp.zeros((EXTRA - 4, 2 * planes), jnp.float32),
                ],
                axis=0,
            ),
        ],
        axis=0,
    )
    high = whole.astype(jnp.bfloat16)
    low = (whole - high.astype(jnp.float32)).astype(jnp.bfloat16)
    tall = 2 * planes + EXTRA
    weights[:tall] = high
    weights[tall:] = low
    for side, pick in ((0, at_column == 0), (1, at_column == last)):
        for part, values in ((0, real), (1, imag)):
            picked = jnp.sum(jnp.where(pick, values, 0.0), axis=1, keepdims=True)
            column[side, part] = jnp.broadcast_to(picked, (planes, 128))
    for part, values in ((0, real), (1, imag)):
        for side, pick in ((0, (at_row == last) & (at_column == 0)), (1, (at_row == 0) & (at_column == last))):
            picked = jnp.sum(jnp.sum(jnp.where(pick, values, 0.0), axis=1, keepdims=True), axis=0, keepdims=True)
            coeff[side, part] = jnp.broadcast_to(picked, (half, 128))

    def solve(s, r):
        load(s, r).wait()
        values = held[s, r].reshape(2 * planes, width)
        upper = values.astype(jnp.bfloat16)
        lower = (values - upper.astype(jnp.float32)).astype(jnp.bfloat16)
        first = jnp.dot(weights[...], upper, preferred_element_type=jnp.float32)
        second = jnp.dot(weights[:tall], lower, preferred_element_type=jnp.float32)
        total = first[:tall] + first[tall:] + second
        solved[s, r] = total[: 2 * planes].reshape(2, planes, width)
        side = s // half
        for part in range(2):
            row = jnp.where(
                side == 0,
                total[2 * planes + part : 2 * planes + part + 1],
                total[2 * planes + 2 + part : 2 * planes + 3 + part],
            )
            base[side, part, r + 2, pl.ds(s % half, 1), :] = row

    cut = planes - RELAY

    def piece(k, to_next, stop=planes):
        s, a, part = k // 4, (k % 4) // 2, k % 2
        row, at = (3 - a, 1 - a) if to_next else (a, 2 + a)
        return pltpu.make_async_remote_copy(
            src_ref=solved.at[s, row, part, pl.ds(0, stop)],
            dst_ref=halo.at[s, at, part, pl.ds(0, stop)],
            send_sem=bulk_send.at[int(to_next), k],
            recv_sem=bulk_recv.at[int(to_next), k],
            device_id=(d, l + 1 if to_next else l - 1),
            device_id_type=MESH,
        )

    relays = (
        (0, 0, (at_pair == 3) | ((at_pair == 7) & has_next), -1),
        (0, 1, (at_pair == 2) | ((at_pair == 6) & (l + 2 < tiles)), jnp.where(at_pair == 6, 7, -1)),
        (0, 2, (at_pair == 1) | ((at_pair == 5) & (l > 5)), jnp.where(at_pair == 5, -5, 3)),
        (1, 0, (at_pair == 4) | ((at_pair == 0) & has_prev), 1),
        (1, 1, (at_pair == 5) | ((at_pair == 1) & (l > 1)), jnp.where(at_pair == 1, -7, 1)),
        (1, 2, (at_pair == 6) | ((at_pair == 2) & (l + 6 < tiles)), jnp.where(at_pair == 2, 5, -3)),
    )
    relay_by = {(way, stage): by for way, stage, _, by in relays}

    def relay(way, stage):
        if stage == 0:
            kept = solved.at[0, 0 if way else rows - 1, 0, pl.ds(cut, RELAY)]
        else:
            kept = passed.at[way, stage - 1]
        there = halo.at[0, 2 if way else 1, 0, pl.ds(cut, RELAY)] if stage == 2 else passed.at[way, stage]
        return pltpu.make_async_remote_copy(
            src_ref=kept,
            dst_ref=there,
            send_sem=relay_send.at[way, stage],
            recv_sem=relay_recv.at[way, stage],
            device_id=(d, l + relay_by[way, stage]),
            device_id_type=MESH,
        )

    def relay_on(stage):
        for way, at, here, _ in relays:
            if at == stage:

                @pl.when(here)
                def _():
                    if stage > 0:
                        relay(way, stage - 1).wait_recv()
                    relay(way, stage).start()

    def send_pieces(start, stop):
        for to_next, there in ((False, has_prev), (True, has_next)):

            @pl.when(there)
            def _():
                def step(k, carry):
                    piece(k, to_next).start()
                    return carry

                lax.fori_loop(start, stop, step, 0)

    def send_first(to_next, there, stop):
        @pl.when(there)
        def _():
            piece(0, to_next, stop).start()
            for k in range(1, PIECES_FIRST):
                piece(k, to_next).start()

    solve(0, 0)
    solve(0, 3)

    def tell_layers():
        for there, by_d in ((has_above, -1), (has_below, 1)):

            @pl.when(there)
            def _():
                pl.semaphore_signal(ready_sem, inc=1, device_id=(d + by_d, l), device_id_type=MESH)

    @pl.when(jnp.logical_not(seam))
    def _():
        pl.semaphore_wait(barrier, tiles_beside + tiles_beyond + layers_beside)
        for there, by_l in ((has_prev & seam_at(l - 1), -1), (has_next & seam_at(l + 1), 1)):

            @pl.when(there)
            def _():
                pl.semaphore_signal(near_sem, inc=1, device_id=(d, l + by_l), device_id_type=MESH)

    @pl.when(seam)
    def _():
        pl.semaphore_wait(near_sem, 1)

    near_prev = has_prev & jnp.logical_not(seam_prev)
    near_next = has_next & jnp.logical_not(seam_next)
    send_first(False, near_prev, planes)
    send_first(True, near_next, planes)

    @pl.when(jnp.logical_not(seam))
    def _():
        tell_layers()

    @pl.when(seam)
    def _():
        pl.semaphore_wait(barrier, 1)

    send_first(False, seam_prev, cut)
    send_first(True, seam_next, cut)
    relay_on(0)
    solve(0, 1)
    solve(0, 2)
    send_pieces(PIECES_FIRST, PIECES_SOLVE)

    def solve_shot(s, carry):
        for r in range(rows):
            solve(s, r)
        return carry

    lax.fori_loop(1, shots, solve_shot, 0)

    def base_copy(side, to_next):
        source_at, target_at = (4, 0) if to_next else (2, 6)
        return pltpu.make_async_remote_copy(
            src_ref=base.at[side, :, pl.ds(source_at, 2)],
            dst_ref=base.at[side, :, pl.ds(target_at, 2)],
            send_sem=base_send.at[int(to_next), side],
            recv_sem=base_recv.at[int(to_next), side],
            device_id=(d, l + 1 if to_next else l - 1),
            device_id_type=MESH,
        )

    base_copies = tuple(
        (needed, to_next, side)
        for needed, side in ((True, side_one), (inner, side_two))
        for to_next in (False, True)
    )

    def both(needed, there):
        return there if needed is True else needed & there

    @pl.when(jnp.logical_not(seam))
    def _():
        pl.semaphore_wait(ready_sem, layers_beside)

    for needed, to_next, side in base_copies:

        @pl.when(both(needed, has_next if to_next else has_prev))
        def _():
            base_copy(side, to_next).start()

    @pl.when(inner)
    def _():
        send_pieces(PIECES_SOLVE, PIECES_SOLVE + PIECES_BASE_INNER)

    @pl.when(jnp.logical_not(inner))
    def _():
        send_pieces(PIECES_SOLVE, PIECES_SOLVE + PIECES_BASE_OUTER)

    small[1].wait()
    small[2].wait()
    for r in range(rows):
        load_cells(r).wait()

        def look_up(i, carry):
            at = pl.ds(pl.multiple_of(i * BLOCK, BLOCK), BLOCK)
            kinds = cells[r, at, :]
            re = jnp.full(kinds.shape, table_re[0], jnp.float32)
            im = jnp.full(kinds.shape, table_im[0], jnp.float32)
            for kind in range(1, CLASSES):
                hit = kinds == kind
                re = jnp.where(hit, table_re[kind], re)
                im = jnp.where(hit, table_im[kind], im)
            kappa[r, 0, at, :] = re
            kappa[r, 1, at, :] = im
            bottom = lax.broadcasted_iota(jnp.int32, kinds.shape, 0) + i * BLOCK == last
            return (carry[0] + jnp.where(bottom, re, 0.0), carry[1] + jnp.where(bottom, im, 0.0))

        zeros = jnp.zeros((BLOCK, width), jnp.float32)
        sums = lax.fori_loop(0, planes // BLOCK, look_up, (zeros, zeros))
        for part in range(2):
            plane[0, part, r] = jnp.broadcast_to(jnp.sum(sums[part], axis=0, keepdims=True), (half, width))
            plane[1, part, r] = jnp.broadcast_to(kappa[r, part, pl.ds(0, 1), :], (half, width))

    for needed, to_next, side in base_copies:

        @pl.when(both(needed, has_prev if to_next else has_next))
        def _():
            base_copy(side, to_next).wait_recv()

    @pl.when(seam)
    def _():
        tell_layers()
        pl.semaphore_wait(ready_sem, layers_beside)

    relay_on(1)

    def lateral(values, r):
        at = r + 2
        return (
            NEAR * (values[at - 1] + values[at + 1])
            + FAR * (values[at - 2] + values[at + 2])
            + along_y(values[at])
            - 5.0 * values[at]
        )

    def trace_copies(side):
        to = d + 1 - 2 * side
        return (
            (
                True,
                True,
                lambda: pltpu.make_async_remote_copy(
                    src_ref=outbound.at[side],
                    dst_ref=inbound.at[side, :, pl.ds(2, 4)],
                    send_sem=trace_send.at[side, 0],
                    recv_sem=trace_recv.at[side, 0],
                    device_id=(to, l),
                    device_id_type=MESH,
                ),
            ),
            (
                has_prev,
                has_next,
                lambda: pltpu.make_async_remote_copy(
                    src_ref=outbound.at[side, :, pl.ds(0, 2)],
                    dst_ref=inbound.at[side, :, pl.ds(6, 2)],
                    send_sem=trace_send.at[side, 1],
                    recv_sem=trace_recv.at[side, 1],
                    device_id=(to, l - 1),
                    device_id_type=MESH,
                ),
            ),
            (
                has_next,
                has_prev,
                lambda: pltpu.make_async_remote_copy(
                    src_ref=outbound.at[side, :, pl.ds(2, 2)],
                    dst_ref=inbound.at[side, :, pl.ds(0, 2)],
                    send_sem=trace_send.at[side, 2],
                    recv_sem=trace_recv.at[side, 2],
                    device_id=(to, l + 1),
                    device_id_type=MESH,
                ),
            ),
        )

    def under(there, act):
        if there is True:
            act()
        else:
            pl.when(there)(act)

    def emit(side):
        factor = [
            jnp.concatenate([coeff[side, part]] * (width // 128), axis=1) for part in range(2)
        ]
        planar = ([], [])
        for row in range(rows + 4):
            t_re, t_im = inbound[side, 0, row], inbound[side, 1, row]
            planar[0].append(base[side, 0, row] + factor[0] * t_re - factor[1] * t_im)
            planar[1].append(base[side, 1, row] + factor[0] * t_im + factor[1] * t_re)
        for r in range(rows):
            re, im = planar[0][r + 2], planar[1][r + 2]
            k_re, k_im = plane[side, 0, r], plane[side, 1, r]
            outbound[side, 0, r] = re + CORRECTION * (lateral(planar[0], r) + k_re * re - k_im * im)
            outbound[side, 1, r] = im + CORRECTION * (lateral(planar[1], r) + k_re * im + k_im * re)
        for goes, _, copy in trace_copies(side):
            under(goes, lambda: copy().start())

    def take(side):
        for _, comes, copy in trace_copies(side):
            under(comes, lambda: copy().wait_recv())

    @pl.when(inner)
    def _():
        take(side_one)

    emit(side_one)
    sent_inner = PIECES_SOLVE + PIECES_BASE_INNER

    @pl.when(inner)
    def _():
        send_pieces(sent_inner, sent_inner + PIECES_TRACE)

    @pl.when(jnp.logical_not(inner))
    def _():
        send_pieces(PIECES_SOLVE + PIECES_BASE_OUTER, pieces - HELD_BACK)

    take(side_two)

    @pl.when(inner)
    def _():
        emit(side_two)

    relay_on(2)

    @pl.when(inner)
    def _():
        send_pieces(sent_inner + PIECES_TRACE, pieces)

    @pl.when(jnp.logical_not(inner))
    def _():
        send_pieces(pieces - HELD_BACK, pieces)

    for side in range(2):
        for part in range(2):
            values = [inbound[side, part, row] for row in range(rows + 4)]
            for r in range(rows):
                spread[side, part, r] = values[r + 2] + CORRECTION * lateral(values, r)

    def own_rows(s, carry):
        side, shot = s // half, s % half
        for r in range(rows):
            t = [inbound[side, part, r + 2, pl.ds(shot, 1), :] for part in range(2)]
            e = [spread[side, part, r, pl.ds(shot, 1), :] for part in range(2)]

            def block(i, inside):
                at = pl.ds(pl.multiple_of(i * BLOCK, BLOCK), BLOCK)
                g_re, g_im = (
                    jnp.concatenate([column[side, part, at, :]] * (width // 128), axis=1) for part in range(2)
                )
                linear, values = [], []
                for part in range(2):
                    v = solved[s, r, part, at, :]
                    near = [solved[s, q, part, at, :] for q in (r - 1, r + 1) if 0 <= q < rows]
                    far = [solved[s, q, part, at, :] for q in (r - 2, r + 2) if 0 <= q < rows]
                    total = along_y(v) - 5.0 * v + NEAR * sum(near[1:], near[0]) + FAR * sum(far[1:], far[0])
                    linear.append(v + CORRECTION * total)
                    values.append(v)
                v_re = values[0] + g_re * t[0] - g_im * t[1]
                v_im = values[1] + g_re * t[1] + g_im * t[0]
                k_re, k_im = kappa[r, 0, at, :], kappa[r, 1, at, :]
                field[s, r, 0, at, :] = (
                    linear[0] + g_re * e[0] - g_im * e[1] + CORRECTION * (k_re * v_re - k_im * v_im)
                )
                field[s, r, 1, at, :] = (
                    linear[1] + g_re * e[1] + g_im * e[0] + CORRECTION * (k_re * v_im + k_im * v_re)
                )
                return inside

            lax.fori_loop(0, planes // BLOCK, block, 0)
        return carry

    lax.fori_loop(0, shots, own_rows, 0)

    def add_rows(s, part, q, to_rows, start=0, stop=planes):
        for first in range(start, stop, BLOCK):
            at = pl.ds(first, min(BLOCK, stop - first))
            v = halo[s, q, part, at, :]
            for r, weight in to_rows:
                field[s, r, part, at, :] = field[s, r, part, at, :] + (CORRECTION * weight) * v

    for needed, to_next, side in base_copies:

        @pl.when(both(needed, has_next if to_next else has_prev))
        def _():
            base_copy(side, to_next).wait_send()

    for goes, _, copy in trace_copies(side_one):
        under(goes, lambda: copy().wait_send())

    @pl.when(inner)
    def _():
        for goes, _, copy in trace_copies(side_two):
            under(goes, lambda: copy().wait_send())

    from_next = (((3, NEAR), (2, FAR)), ((3, FAR),))
    from_prev = (((0, NEAR), (1, FAR)), ((0, FAR),))

    def add_piece(s, a, part, stop_prev, stop_next):
        k = s * 4 + a * 2 + part
        for there, to_next, stop, q, to_rows in (
            (has_next, True, stop_next, 2 + a, from_next[a]),
            (has_prev, False, stop_prev, 1 - a, from_prev[a]),
        ):

            @pl.when(there)
            def _():
                piece(k, not to_next, stop).wait_recv()
                piece(k, to_next, stop).wait_send()
                add_rows(s, part, q, to_rows, 0, stop)

    def add_shot(s, carry):
        for a in range(2):
            for part in range(2):
                add_piece(s, a, part, planes, planes)
        return carry

    def add_first(to_next, there, stop):
        @pl.when(there)
        def _():
            piece(0, not to_next, stop).wait_recv()
            piece(0, to_next, stop).wait_send()
            add_rows(0, 0, 2 if to_next else 1, (from_next if to_next else from_prev)[0], 0, stop)

    add_first(True, near_next, planes)
    add_first(False, near_prev, planes)
    add_first(True, seam_next, cut)
    add_first(False, seam_prev, cut)
    for a, part in ((0, 1), (1, 0), (1, 1)):
        add_piece(0, a, part, planes, planes)
    lax.fori_loop(1, shots - 1, add_shot, 0)
    for way, stage, here, _ in relays:

        @pl.when(here)
        def _():
            relay(way, stage).wait_send()

    for to_next, there in ((True, seam_next), (False, seam_prev)):

        @pl.when(there)
        def _():
            relay(1 if to_next else 0, 2).wait_recv()
            add_rows(0, 0, 2 if to_next else 1, (from_next if to_next else from_prev)[0], cut, planes)

    add_shot(shots - 1, 0)


def write_kernel(field, out, sem):
    shots, rows = field.shape[:2]

    def copy(s, r):
        return pltpu.make_async_copy(field.at[s, r], out.at[s, :, :, r, :], sem.at[s, r])

    for s in range(shots):
        for r in range(rows):
            copy(s, r).start()
    for s in range(shots):
        for r in range(rows):
            copy(s, r).wait()


def on_device(source, line_inverse, plane_count, classes, table_re, table_im):
    shots, parts, planes, rows, width = source.shape
    half = shots // 2
    by_rows = (shots, rows, parts, planes, width)
    any_space = pl.BlockSpec(memory_space=pl.ANY)
    hbm = pl.BlockSpec(memory_space=pltpu.HBM)
    vmem = pl.BlockSpec(memory_space=pltpu.VMEM)
    tall = 2 * planes + EXTRA
    pieces = shots * 4
    dma = pltpu.SemaphoreType.DMA
    operands = (source, line_inverse, classes, table_re, table_im)
    field = pl.pallas_call(
        field_kernel,
        out_shape=jax.ShapeDtypeStruct(by_rows, jnp.float32),
        in_specs=[pl.BlockSpec(memory_space=pltpu.SMEM)] + [hbm] * len(operands),
        out_specs=vmem,
        scratch_shapes=[
            pltpu.VMEM((parts, planes, planes), jnp.float32),
            pltpu.SMEM((CLASSES,), jnp.float32),
            pltpu.SMEM((CLASSES,), jnp.float32),
            pltpu.VMEM(by_rows, jnp.float32),
            pltpu.VMEM((rows, planes, width), jnp.int32),
            pltpu.VMEM(by_rows, jnp.float32),
            pltpu.VMEM((shots, 4, parts, planes, width), jnp.float32),
            pltpu.VMEM((rows, parts, planes, width), jnp.float32),
            pltpu.VMEM((2, parts, rows, half, width), jnp.float32),
            pltpu.VMEM((2, parts, rows + 4, half, width), jnp.float32),
            pltpu.VMEM((2, parts, rows + 4, half, width), jnp.float32),
            pltpu.VMEM((2, parts, rows, half, width), jnp.float32),
            pltpu.VMEM((2, parts, rows, half, width), jnp.float32),
            pltpu.VMEM((2, parts, planes, 128), jnp.float32),
            pltpu.VMEM((2, parts, half, 128), jnp.float32),
            pltpu.VMEM((2 * tall, 2 * planes), jnp.bfloat16),
            dma((3,)),
            dma((shots, rows)),
            dma((rows,)),
            dma((2, pieces)),
            dma((2, pieces)),
            dma((2, 2)),
            dma((2, 2)),
            dma((2, 3)),
            dma((2, 3)),
            pltpu.SemaphoreType.REGULAR,
            pltpu.SemaphoreType.REGULAR,
            dma((2, 3)),
            dma((2, 3)),
            pltpu.VMEM((2, 2, RELAY, width), jnp.float32),
        ],
        compiler_params=pltpu.CompilerParams(
            collective_id=0, has_side_effects=True, vmem_limit_bytes=40 * 2**20
        ),
    )(plane_count, *(pltpu.with_memory_space_constraint(x, pltpu.HBM) for x in operands))
    return pl.pallas_call(
        write_kernel,
        out_shape=jax.ShapeDtypeStruct(source.shape, jnp.float32),
        in_specs=[vmem],
        out_specs=any_space,
        scratch_shapes=[dma((shots, rows))],
        compiler_params=pltpu.CompilerParams(vmem_limit_bytes=8 * 2**20),
    )(field)


def solution(mesh):
    in_specs = (
        P(None, None, "depth", "lat", None),
        P("depth", None, None, None),
        P("depth"),
        P("depth", "lat", None),
        P(),
        P(),
    )
    out_specs = P(None, None, "depth", "lat", None)
    return jax.shard_map(
        on_device, mesh=mesh, in_specs=in_specs, out_specs=out_specs, check_vma=False
    )
```

```python
import functools

import jax
import jax.numpy as jnp
from jax import lax
from jax.experimental import pallas as pl
from jax.experimental.pallas import tpu as pltpu
from jax.sharding import PartitionSpec as P

MESH = pl.DeviceIdType.MESH
CLASSES = 16
CORRECTION = 0.1
NEAR = 4.0 / 3.0
FAR = -1.0 / 12.0
BLOCK = 16
EXTRA = 16
RING = 4
RELAY = 48
PIECES = (
    (0, 0, 1, 0, 1),
    (0, 0, 1, 1, 1),
    (0, 1, 1, 0, 1),
    (0, 1, 1, 1, 1),
    (1, 0, 1, 0, 2),
    (1, 1, 1, 0, 2),
    (2, 0, 2, 0, 2),
    (3, 0, 1, 0, 2),
    (3, 1, 1, 0, 1),
    (3, 1, 1, 1, 1),
)
AFTER_FIRST = 2
AFTER_SHOT = 3
AFTER_BASE_OUTER = 5
AFTER_BASE_INNER = 5
AFTER_TRACE_INNER = 6
AFTER_TRACE_OUTER = 7


def along_y(x):
    size = x.shape[1]
    lane = lax.broadcasted_iota(jnp.int32, x.shape, 1)
    near = jnp.where(lane >= 1, pltpu.roll(x, 1, 1), 0.0) + jnp.where(
        lane < size - 1, pltpu.roll(x, size - 1, 1), 0.0
    )
    far = jnp.where(lane >= 2, pltpu.roll(x, 2, 1), 0.0) + jnp.where(
        lane < size - 2, pltpu.roll(x, size - 2, 1), 0.0
    )
    return NEAR * near + FAR * far


def field_kernel(
    count, source, matrix_from, classes, table_re_from, table_im_from, field,
    matrix, table_re, table_im,
    held, cells, solved, halo, kappa, plane, base, inbound, outbound, spread, column, coeff, weights,
    small_sem, load_sem, cell_sem, bulk_send, bulk_recv, base_send, base_recv, trace_send, trace_recv,
    ready_sem, near_sem, relay_send, relay_recv, passed,
):
    shots, rows, _, planes, width = held.shape
    half = shots // 2
    d = lax.axis_index("depth")
    l = lax.axis_index("lat")
    layers = lax.axis_size("depth")
    tiles = lax.axis_size("lat")
    has_prev = l > 0
    has_next = l < tiles - 1
    has_above = d > 0
    has_below = d < layers - 1
    inner = has_above & has_below
    seam_prev = has_prev & (l % RING == 0)
    seam_next = has_next & (l % RING == RING - 1)
    seam = seam_prev | seam_next
    at_pair = l % (2 * RING)

    def seam_at(tile):
        at = tile % RING
        return ((tile > 0) & (at == 0)) | ((tile < tiles - 1) & (at == RING - 1))

    side_one = jnp.where(d >= layers // 2, 1, 0)
    side_two = 1 - side_one

    def load(s, r):
        return pltpu.make_async_copy(source.at[s, :, :, r, :], held.at[s, r], load_sem.at[s, r])

    def load_cells(r):
        return pltpu.make_async_copy(classes.at[:, r, :], cells.at[r], cell_sem.at[r])

    small = [
        pltpu.make_async_copy(here, there, small_sem.at[i])
        for i, (here, there) in enumerate(
            ((matrix_from.at[0], matrix), (table_re_from, table_re), (table_im_from, table_im))
        )
    ]
    barrier = pltpu.get_barrier_semaphore()
    for there, by_d, by_l in (
        (has_prev & (seam | jnp.logical_not(seam_at(l - 1))), 0, -1),
        (has_next & (seam | jnp.logical_not(seam_at(l + 1))), 0, 1),
        (has_above & jnp.logical_not(seam), -1, 0),
        (has_below & jnp.logical_not(seam), 1, 0),
        ((at_pair == 5) & (l > 5), 0, -7),
        ((at_pair == 2) & (l + 6 < tiles), 0, 7),
    ):

        @pl.when(there)
        def _():
            pl.semaphore_signal(barrier, inc=1, device_id=(d + by_d, l + by_l), device_id_type=MESH)

    layers_beside = jnp.where(has_above, 1, 0) + jnp.where(has_below, 1, 0)
    tiles_beside = jnp.where(has_prev, 1, 0) + jnp.where(has_next, 1, 0)
    tiles_beyond = jnp.where(((at_pair == 6) & (l + 2 < tiles)) | ((at_pair == 1) & (l > 1)), 1, 0)

    small[0].start()
    for r in (0, 3, 1, 2):
        load(0, r).start()
    small[1].start()
    small[2].start()
    for s in range(1, shots):
        for r in range(rows):
            load(s, r).start()
    for r in range(rows):
        load_cells(r).start()

    for there, at in ((has_prev, pl.ds(0, 2)), (has_next, pl.ds(6, 2))):

        @pl.when(jnp.logical_not(there))
        def _():
            base[:, :, at] = jnp.zeros((2, 2, 2, half, width), jnp.float32)
            inbound[:, :, at] = jnp.zeros((2, 2, 2, half, width), jnp.float32)

    for there, side in ((has_above, 0), (has_below, 1)):

        @pl.when(jnp.logical_not(there))
        def _():
            inbound[side] = jnp.zeros(inbound.shape[1:], jnp.float32)

    small[0].wait()
    last = count[0] - 1
    at_row = lax.broadcasted_iota(jnp.int32, (planes, planes), 0)
    at_column = lax.broadcasted_iota(jnp.int32, (planes, planes), 1)
    live = (at_row <= last) & (at_column <= last)
    real = jnp.where(live, matrix[0], 0.0)
    imag = jnp.where(live, matrix[1], 0.0)
    end_re = jnp.sum(jnp.where(at_row == last, real, 0.0), axis=0, keepdims=True)
    end_im = jnp.sum(jnp.where(at_row == last, imag, 0.0), axis=0, keepdims=True)
    whole = jnp.concatenate(
        [
            jnp.concatenate([real, -imag], axis=1),
            jnp.concatenate([imag, real], axis=1),
            jnp.concatenate(
                [
                    jnp.concatenate([end_re, -end_im], axis=1),
                    jnp.concatenate([end_im, end_re], axis=1),
                    jnp.concatenate([real[:1], -imag[:1]], axis=1),
                    jnp.concatenate([imag[:1], real[:1]], axis=1),
                    jnp.zeros((EXTRA - 4, 2 * planes), jnp.float32),
                ],
                axis=0,
            ),
        ],
        axis=0,
    )
    high = whole.astype(jnp.bfloat16)
    low = (whole - high.astype(jnp.float32)).astype(jnp.bfloat16)
    tall = 2 * planes + EXTRA
    weights[:tall] = high
    weights[tall:] = low
    for side, pick in ((0, at_column == 0), (1, at_column == last)):
        for part, values in ((0, real), (1, imag)):
            picked = jnp.sum(jnp.where(pick, values, 0.0), axis=1, keepdims=True)
            column[side, part] = jnp.broadcast_to(picked, (planes, 128))
    for part, values in ((0, real), (1, imag)):
        for side, pick in ((0, (at_row == last) & (at_column == 0)), (1, (at_row == 0) & (at_column == last))):
            picked = jnp.sum(jnp.sum(jnp.where(pick, values, 0.0), axis=1, keepdims=True), axis=0, keepdims=True)
            coeff[side, part] = jnp.broadcast_to(picked, (half, 128))

    def solve(s, r):
        load(s, r).wait()
        values = held[s, r].reshape(2 * planes, width)
        upper = values.astype(jnp.bfloat16)
        lower = (values - upper.astype(jnp.float32)).astype(jnp.bfloat16)
        first = jnp.dot(weights[...], upper, preferred_element_type=jnp.float32)
        second = jnp.dot(weights[:tall], lower, preferred_element_type=jnp.float32)
        total = first[:tall] + first[tall:] + second
        solved[s, r] = total[: 2 * planes].reshape(2, planes, width)
        side = s // half
        for part in range(2):
            row = jnp.where(
                side == 0,
                total[2 * planes + part : 2 * planes + part + 1],
                total[2 * planes + 2 + part : 2 * planes + 3 + part],
            )
            base[side, part, r + 2, pl.ds(s % half, 1), :] = row

    cut = planes - RELAY

    def piece(k, to_next, stop=planes):
        s, a, count_rows, part, parts = PIECES[k]
        row, at = (rows - a - count_rows, 2 - a - count_rows) if to_next else (a, 2 + a)
        return pltpu.make_async_remote_copy(
            src_ref=solved.at[s, pl.ds(row, count_rows), pl.ds(part, parts), pl.ds(0, stop)],
            dst_ref=halo.at[s, pl.ds(at, count_rows), pl.ds(part, parts), pl.ds(0, stop)],
            send_sem=bulk_send.at[int(to_next), k],
            recv_sem=bulk_recv.at[int(to_next), k],
            device_id=(d, l + 1 if to_next else l - 1),
            device_id_type=MESH,
        )

    relays = (
        (0, 0, (at_pair == 3) | ((at_pair == 7) & has_next), -1),
        (0, 1, (at_pair == 2) | ((at_pair == 6) & (l + 2 < tiles)), jnp.where(at_pair == 6, 7, -1)),
        (0, 2, (at_pair == 1) | ((at_pair == 5) & (l > 5)), jnp.where(at_pair == 5, -5, 3)),
        (1, 0, (at_pair == 4) | ((at_pair == 0) & has_prev), 1),
        (1, 1, (at_pair == 5) | ((at_pair == 1) & (l > 1)), jnp.where(at_pair == 1, -7, 1)),
        (1, 2, (at_pair == 6) | ((at_pair == 2) & (l + 6 < tiles)), jnp.where(at_pair == 2, 5, -3)),
    )
    relay_by = {(way, stage): by for way, stage, _, by in relays}

    def relay(way, stage):
        if stage == 0:
            kept = solved.at[0, 0 if way else rows - 1, 0, pl.ds(cut, RELAY)]
        else:
            kept = passed.at[way, stage - 1]
        there = halo.at[0, 2 if way else 1, 0, pl.ds(cut, RELAY)] if stage == 2 else passed.at[way, stage]
        return pltpu.make_async_remote_copy(
            src_ref=kept,
            dst_ref=there,
            send_sem=relay_send.at[way, stage],
            recv_sem=relay_recv.at[way, stage],
            device_id=(d, l + relay_by[way, stage]),
            device_id_type=MESH,
        )

    def relay_on(stage):
        for way, at, here, _ in relays:
            if at == stage:

                @pl.when(here)
                def _():
                    if stage > 0:
                        relay(way, stage - 1).wait_recv()
                    relay(way, stage).start()

    def send_pieces(start, stop):
        for to_next, there in ((False, has_prev), (True, has_next)):

            @pl.when(there)
            def _():
                for k in range(start, stop):
                    piece(k, to_next).start()

    def send_first(to_next, there, stop):
        @pl.when(there)
        def _():
            piece(0, to_next, stop).start()
            for k in range(1, AFTER_FIRST):
                piece(k, to_next).start()

    solve(0, 0)
    solve(0, 3)

    def tell_layers():
        for there, by_d in ((has_above, -1), (has_below, 1)):

            @pl.when(there)
            def _():
                pl.semaphore_signal(ready_sem, inc=1, device_id=(d + by_d, l), device_id_type=MESH)

    @pl.when(jnp.logical_not(seam))
    def _():
        pl.semaphore_wait(barrier, tiles_beside + tiles_beyond + layers_beside)
        for there, by_l in ((has_prev & seam_at(l - 1), -1), (has_next & seam_at(l + 1), 1)):

            @pl.when(there)
            def _():
                pl.semaphore_signal(near_sem, inc=1, device_id=(d, l + by_l), device_id_type=MESH)

    @pl.when(seam)
    def _():
        pl.semaphore_wait(near_sem, 1)

    near_prev = has_prev & jnp.logical_not(seam_prev)
    near_next = has_next & jnp.logical_not(seam_next)
    send_first(False, near_prev, planes)
    send_first(True, near_next, planes)

    @pl.when(jnp.logical_not(seam))
    def _():
        tell_layers()

    @pl.when(seam)
    def _():
        pl.semaphore_wait(barrier, 1)

    send_first(False, seam_prev, cut)
    send_first(True, seam_next, cut)
    relay_on(0)
    solve(0, 1)
    solve(0, 2)
    send_pieces(AFTER_FIRST, AFTER_SHOT)

    def solve_shot(s, carry):
        for r in range(rows):
            solve(s, r)
        return carry

    lax.fori_loop(1, shots, solve_shot, 0)

    def base_copy(side, to_next):
        source_at, target_at = (4, 0) if to_next else (2, 6)
        return pltpu.make_async_remote_copy(
            src_ref=base.at[side, :, pl.ds(source_at, 2)],
            dst_ref=base.at[side, :, pl.ds(target_at, 2)],
            send_sem=base_send.at[int(to_next), side],
            recv_sem=base_recv.at[int(to_next), side],
            device_id=(d, l + 1 if to_next else l - 1),
            device_id_type=MESH,
        )

    base_copies = tuple(
        (needed, to_next, side)
        for needed, side in ((True, side_one), (inner, side_two))
        for to_next in (False, True)
    )

    def both(needed, there):
        return there if needed is True else needed & there

    @pl.when(jnp.logical_not(seam))
    def _():
        pl.semaphore_wait(ready_sem, layers_beside)

    for needed, to_next, side in base_copies:

        @pl.when(both(needed, has_next if to_next else has_prev))
        def _():
            base_copy(side, to_next).start()

    @pl.when(inner)
    def _():
        send_pieces(AFTER_SHOT, AFTER_BASE_INNER)

    @pl.when(jnp.logical_not(inner))
    def _():
        send_pieces(AFTER_SHOT, AFTER_BASE_OUTER)

    small[1].wait()
    small[2].wait()
    for r in range(rows):
        load_cells(r).wait()

        def look_up(i, carry):
            at = pl.ds(pl.multiple_of(i * BLOCK, BLOCK), BLOCK)
            kinds = cells[r, at, :]
            re = jnp.full(kinds.shape, table_re[0], jnp.float32)
            im = jnp.full(kinds.shape, table_im[0], jnp.float32)
            for kind in range(1, CLASSES):
                hit = kinds == kind
                re = jnp.where(hit, table_re[kind], re)
                im = jnp.where(hit, table_im[kind], im)
            kappa[r, 0, at, :] = re
            kappa[r, 1, at, :] = im
            bottom = lax.broadcasted_iota(jnp.int32, kinds.shape, 0) + i * BLOCK == last
            return (carry[0] + jnp.where(bottom, re, 0.0), carry[1] + jnp.where(bottom, im, 0.0))

        zeros = jnp.zeros((BLOCK, width), jnp.float32)
        sums = lax.fori_loop(0, planes // BLOCK, look_up, (zeros, zeros))
        for part in range(2):
            plane[0, part, r] = jnp.broadcast_to(jnp.sum(sums[part], axis=0, keepdims=True), (half, width))
            plane[1, part, r] = jnp.broadcast_to(kappa[r, part, pl.ds(0, 1), :], (half, width))

    for needed, to_next, side in base_copies:

        @pl.when(both(needed, has_prev if to_next else has_next))
        def _():
            base_copy(side, to_next).wait_recv()

    @pl.when(seam)
    def _():
        tell_layers()
        pl.semaphore_wait(ready_sem, layers_beside)

    relay_on(1)

    def lateral(values, r):
        at = r + 2
        return (
            NEAR * (values[at - 1] + values[at + 1])
            + FAR * (values[at - 2] + values[at + 2])
            + along_y(values[at])
            - 5.0 * values[at]
        )

    def trace_copies(side):
        to = d + 1 - 2 * side
        return (
            (
                True,
                True,
                lambda: pltpu.make_async_remote_copy(
                    src_ref=outbound.at[side],
                    dst_ref=inbound.at[side, :, pl.ds(2, 4)],
                    send_sem=trace_send.at[side, 0],
                    recv_sem=trace_recv.at[side, 0],
                    device_id=(to, l),
                    device_id_type=MESH,
                ),
            ),
            (
                has_prev,
                has_next,
                lambda: pltpu.make_async_remote_copy(
                    src_ref=outbound.at[side, :, pl.ds(0, 2)],
                    dst_ref=inbound.at[side, :, pl.ds(6, 2)],
                    send_sem=trace_send.at[side, 1],
                    recv_sem=trace_recv.at[side, 1],
                    device_id=(to, l - 1),
                    device_id_type=MESH,
                ),
            ),
            (
                has_next,
                has_prev,
                lambda: pltpu.make_async_remote_copy(
                    src_ref=outbound.at[side, :, pl.ds(2, 2)],
                    dst_ref=inbound.at[side, :, pl.ds(0, 2)],
                    send_sem=trace_send.at[side, 2],
                    recv_sem=trace_recv.at[side, 2],
                    device_id=(to, l + 1),
                    device_id_type=MESH,
                ),
            ),
        )

    def under(there, act):
        if there is True:
            act()
        else:
            pl.when(there)(act)

    def emit(side):
        factor = [
            jnp.concatenate([coeff[side, part]] * (width // 128), axis=1) for part in range(2)
        ]
        planar = ([], [])
        for row in range(rows + 4):
            t_re, t_im = inbound[side, 0, row], inbound[side, 1, row]
            planar[0].append(base[side, 0, row] + factor[0] * t_re - factor[1] * t_im)
            planar[1].append(base[side, 1, row] + factor[0] * t_im + factor[1] * t_re)
        for r in range(rows):
            re, im = planar[0][r + 2], planar[1][r + 2]
            k_re, k_im = plane[side, 0, r], plane[side, 1, r]
            outbound[side, 0, r] = re + CORRECTION * (lateral(planar[0], r) + k_re * re - k_im * im)
            outbound[side, 1, r] = im + CORRECTION * (lateral(planar[1], r) + k_re * im + k_im * re)
        for goes, _, copy in trace_copies(side):
            under(goes, lambda: copy().start())

    def take(side):
        for _, comes, copy in trace_copies(side):
            under(comes, lambda: copy().wait_recv())

    @pl.when(inner)
    def _():
        take(side_one)

    emit(side_one)

    @pl.when(inner)
    def _():
        send_pieces(AFTER_BASE_INNER, AFTER_TRACE_INNER)

    @pl.when(jnp.logical_not(inner))
    def _():
        send_pieces(AFTER_BASE_OUTER, AFTER_TRACE_OUTER)

    take(side_two)

    @pl.when(inner)
    def _():
        emit(side_two)

    relay_on(2)

    @pl.when(inner)
    def _():
        send_pieces(AFTER_TRACE_INNER, len(PIECES))

    @pl.when(jnp.logical_not(inner))
    def _():
        send_pieces(AFTER_TRACE_OUTER, len(PIECES))

    for side in range(2):
        for part in range(2):
            values = [inbound[side, part, row] for row in range(rows + 4)]
            for r in range(rows):
                spread[side, part, r] = values[r + 2] + CORRECTION * lateral(values, r)

    def own_rows(s, carry):
        side, shot = s // half, s % half
        for r in range(rows):
            t = [inbound[side, part, r + 2, pl.ds(shot, 1), :] for part in range(2)]
            e = [spread[side, part, r, pl.ds(shot, 1), :] for part in range(2)]

            def block(i, inside):
                at = pl.ds(pl.multiple_of(i * BLOCK, BLOCK), BLOCK)
                g_re, g_im = (
                    jnp.concatenate([column[side, part, at, :]] * (width // 128), axis=1) for part in range(2)
                )
                linear, values = [], []
                for part in range(2):
                    v = solved[s, r, part, at, :]
                    near = [solved[s, q, part, at, :] for q in (r - 1, r + 1) if 0 <= q < rows]
                    far = [solved[s, q, part, at, :] for q in (r - 2, r + 2) if 0 <= q < rows]
                    total = along_y(v) - 5.0 * v + NEAR * sum(near[1:], near[0]) + FAR * sum(far[1:], far[0])
                    linear.append(v + CORRECTION * total)
                    values.append(v)
                v_re = values[0] + g_re * t[0] - g_im * t[1]
                v_im = values[1] + g_re * t[1] + g_im * t[0]
                k_re, k_im = kappa[r, 0, at, :], kappa[r, 1, at, :]
                field[s, r, 0, at, :] = (
                    linear[0] + g_re * e[0] - g_im * e[1] + CORRECTION * (k_re * v_re - k_im * v_im)
                )
                field[s, r, 1, at, :] = (
                    linear[1] + g_re * e[1] + g_im * e[0] + CORRECTION * (k_re * v_im + k_im * v_re)
                )
                return inside

            lax.fori_loop(0, planes // BLOCK, block, 0)
        return carry

    lax.fori_loop(0, shots, own_rows, 0)

    def add_rows(s, part, q, to_rows, start=0, stop=planes):
        for first in range(start, stop, BLOCK):
            at = pl.ds(first, min(BLOCK, stop - first))
            v = halo[s, q, part, at, :]
            for r, weight in to_rows:
                field[s, r, part, at, :] = field[s, r, part, at, :] + (CORRECTION * weight) * v

    for needed, to_next, side in base_copies:

        @pl.when(both(needed, has_next if to_next else has_prev))
        def _():
            base_copy(side, to_next).wait_send()

    for goes, _, copy in trace_copies(side_one):
        under(goes, lambda: copy().wait_send())

    @pl.when(inner)
    def _():
        for goes, _, copy in trace_copies(side_two):
            under(goes, lambda: copy().wait_send())

    from_next = (((3, NEAR), (2, FAR)), ((3, FAR),))
    from_prev = (((0, NEAR), (1, FAR)), ((0, FAR),))

    def add_piece(k, to_next, there, stop=planes):
        s, first_row, count_rows, first_part, parts = PIECES[k]

        @pl.when(there)
        def _():
            piece(k, not to_next, stop).wait_recv()
            piece(k, to_next, stop).wait_send()
            for a in range(first_row, first_row + count_rows):
                q, to_rows = (2 + a, from_next[a]) if to_next else (1 - a, from_prev[a])

                def add_part(part, carry):
                    add_rows(s, part, q, to_rows, 0, stop)
                    return carry

                if parts == 1:
                    add_part(first_part, 0)
                else:
                    lax.fori_loop(first_part, first_part + parts, add_part, 0)

    add_piece(0, True, near_next)
    add_piece(0, False, near_prev)
    add_piece(0, True, seam_next, cut)
    add_piece(0, False, seam_prev, cut)
    for k in range(1, AFTER_TRACE_INNER):
        add_piece(k, True, has_next)
        add_piece(k, False, has_prev)
    for way, stage, here, _ in relays:

        @pl.when(here)
        def _():
            relay(way, stage).wait_send()

    for to_next, there in ((True, seam_next), (False, seam_prev)):

        @pl.when(there)
        def _():
            relay(1 if to_next else 0, 2).wait_recv()
            add_rows(0, 0, 2 if to_next else 1, (from_next if to_next else from_prev)[0], cut, planes)

    for k in range(AFTER_TRACE_INNER, len(PIECES)):
        add_piece(k, True, has_next)
        add_piece(k, False, has_prev)


def write_kernel(field, out, sem):
    shots, rows = field.shape[:2]

    def copy(s, r):
        return pltpu.make_async_copy(field.at[s, r], out.at[s, :, :, r, :], sem.at[s, r])

    for s in range(shots):
        for r in range(rows):
            copy(s, r).start()
    for s in range(shots):
        for r in range(rows):
            copy(s, r).wait()


def on_device(source, line_inverse, plane_count, classes, table_re, table_im):
    shots, parts, planes, rows, width = source.shape
    half = shots // 2
    by_rows = (shots, rows, parts, planes, width)
    any_space = pl.BlockSpec(memory_space=pl.ANY)
    hbm = pl.BlockSpec(memory_space=pltpu.HBM)
    vmem = pl.BlockSpec(memory_space=pltpu.VMEM)
    tall = 2 * planes + EXTRA
    pieces = len(PIECES)
    dma = pltpu.SemaphoreType.DMA
    operands = (source, line_inverse, classes, table_re, table_im)
    field = pl.pallas_call(
        field_kernel,
        out_shape=jax.ShapeDtypeStruct(by_rows, jnp.float32),
        in_specs=[pl.BlockSpec(memory_space=pltpu.SMEM)] + [hbm] * len(operands),
        out_specs=vmem,
        scratch_shapes=[
            pltpu.VMEM((parts, planes, planes), jnp.float32),
            pltpu.SMEM((CLASSES,), jnp.float32),
            pltpu.SMEM((CLASSES,), jnp.float32),
            pltpu.VMEM(by_rows, jnp.float32),
            pltpu.VMEM((rows, planes, width), jnp.int32),
            pltpu.VMEM(by_rows, jnp.float32),
            pltpu.VMEM((shots, 4, parts, planes, width), jnp.float32),
            pltpu.VMEM((rows, parts, planes, width), jnp.float32),
            pltpu.VMEM((2, parts, rows, half, width), jnp.float32),
            pltpu.VMEM((2, parts, rows + 4, half, width), jnp.float32),
            pltpu.VMEM((2, parts, rows + 4, half, width), jnp.float32),
            pltpu.VMEM((2, parts, rows, half, width), jnp.float32),
            pltpu.VMEM((2, parts, rows, half, width), jnp.float32),
            pltpu.VMEM((2, parts, planes, 128), jnp.float32),
            pltpu.VMEM((2, parts, half, 128), jnp.float32),
            pltpu.VMEM((2 * tall, 2 * planes), jnp.bfloat16),
            dma((3,)),
            dma((shots, rows)),
            dma((rows,)),
            dma((2, pieces)),
            dma((2, pieces)),
            dma((2, 2)),
            dma((2, 2)),
            dma((2, 3)),
            dma((2, 3)),
            pltpu.SemaphoreType.REGULAR,
            pltpu.SemaphoreType.REGULAR,
            dma((2, 3)),
            dma((2, 3)),
            pltpu.VMEM((2, 2, RELAY, width), jnp.float32),
        ],
        compiler_params=pltpu.CompilerParams(
            collective_id=0, has_side_effects=True, vmem_limit_bytes=40 * 2**20
        ),
    )(plane_count, *(pltpu.with_memory_space_constraint(x, pltpu.HBM) for x in operands))
    return pl.pallas_call(
        write_kernel,
        out_shape=jax.ShapeDtypeStruct(source.shape, jnp.float32),
        in_specs=[vmem],
        out_specs=any_space,
        scratch_shapes=[dma((shots, rows))],
        compiler_params=pltpu.CompilerParams(vmem_limit_bytes=8 * 2**20),
    )(field)


def solution(mesh):
    in_specs = (
        P(None, None, "depth", "lat", None),
        P("depth", None, None, None),
        P("depth"),
        P("depth", "lat", None),
        P(),
        P(),
    )
    out_specs = P(None, None, "depth", "lat", None)
    return jax.shard_map(
        on_device, mesh=mesh, in_specs=in_specs, out_specs=out_specs, check_vma=False
    )
```

```python
import functools

import jax
import jax.numpy as jnp
from jax import lax
from jax.experimental import pallas as pl
from jax.experimental.pallas import tpu as pltpu
from jax.sharding import PartitionSpec as P

MESH = pl.DeviceIdType.MESH
CLASSES = 16
CORRECTION = 0.1
NEAR = 4.0 / 3.0
FAR = -1.0 / 12.0
BLOCK = 16
EXTRA = 16
RING = 4
RELAY = 48
PIECES = (
    (0, 0, 1, 0, 1),
    (0, 0, 1, 1, 1),
    (0, 1, 1, 0, 2),
    (1, 0, 2, 0, 2),
    (2, 0, 2, 0, 2),
    (3, 0, 1, 0, 2),
    (3, 1, 1, 0, 1),
    (3, 1, 1, 1, 1),
)
AFTER_FIRST = 2
AFTER_SHOT = 3
AFTER_BASE_OUTER = 3
AFTER_BASE_INNER = 4
AFTER_TRACE_INNER = 4
AFTER_TRACE_OUTER = 5


def along_y(x):
    size = x.shape[1]
    lane = lax.broadcasted_iota(jnp.int32, x.shape, 1)
    near = jnp.where(lane >= 1, pltpu.roll(x, 1, 1), 0.0) + jnp.where(
        lane < size - 1, pltpu.roll(x, size - 1, 1), 0.0
    )
    far = jnp.where(lane >= 2, pltpu.roll(x, 2, 1), 0.0) + jnp.where(
        lane < size - 2, pltpu.roll(x, size - 2, 1), 0.0
    )
    return NEAR * near + FAR * far


def field_kernel(
    count, source, matrix_from, classes, table_re_from, table_im_from, field,
    matrix, table_re, table_im,
    held, cells, solved, halo, kappa, plane, base, inbound, outbound, spread, column, coeff, weights,
    small_sem, load_sem, cell_sem, bulk_send, bulk_recv, base_send, base_recv, trace_send, trace_recv,
    ready_sem, near_sem, relay_send, relay_recv, passed,
):
    shots, rows, _, planes, width = held.shape
    half = shots // 2
    d = lax.axis_index("depth")
    l = lax.axis_index("lat")
    layers = lax.axis_size("depth")
    tiles = lax.axis_size("lat")
    has_prev = l > 0
    has_next = l < tiles - 1
    has_above = d > 0
    has_below = d < layers - 1
    inner = has_above & has_below
    seam_prev = has_prev & (l % RING == 0)
    seam_next = has_next & (l % RING == RING - 1)
    seam = seam_prev | seam_next
    at_pair = l % (2 * RING)

    def seam_at(tile):
        at = tile % RING
        return ((tile > 0) & (at == 0)) | ((tile < tiles - 1) & (at == RING - 1))

    side_one = jnp.where(d >= layers // 2, 1, 0)
    side_two = 1 - side_one

    def load(s, r):
        return pltpu.make_async_copy(source.at[s, :, :, r, :], held.at[s, r], load_sem.at[s, r])

    def load_cells(r):
        return pltpu.make_async_copy(classes.at[:, r, :], cells.at[r], cell_sem.at[r])

    small = [
        pltpu.make_async_copy(here, there, small_sem.at[i])
        for i, (here, there) in enumerate(
            ((matrix_from.at[0], matrix), (table_re_from, table_re), (table_im_from, table_im))
        )
    ]
    barrier = pltpu.get_barrier_semaphore()
    for there, by_d, by_l in (
        (has_prev & (seam | jnp.logical_not(seam_at(l - 1))), 0, -1),
        (has_next & (seam | jnp.logical_not(seam_at(l + 1))), 0, 1),
        (has_above & jnp.logical_not(seam), -1, 0),
        (has_below & jnp.logical_not(seam), 1, 0),
        ((at_pair == 5) & (l > 5), 0, -7),
        ((at_pair == 2) & (l + 6 < tiles), 0, 7),
    ):

        @pl.when(there)
        def _():
            pl.semaphore_signal(barrier, inc=1, device_id=(d + by_d, l + by_l), device_id_type=MESH)

    layers_beside = jnp.where(has_above, 1, 0) + jnp.where(has_below, 1, 0)
    tiles_beside = jnp.where(has_prev, 1, 0) + jnp.where(has_next, 1, 0)
    tiles_beyond = jnp.where(((at_pair == 6) & (l + 2 < tiles)) | ((at_pair == 1) & (l > 1)), 1, 0)

    small[0].start()
    for r in (0, 3, 1, 2):
        load(0, r).start()
    small[1].start()
    small[2].start()
    for s in range(1, shots):
        for r in range(rows):
            load(s, r).start()
    for r in range(rows):
        load_cells(r).start()

    for there, at in ((has_prev, pl.ds(0, 2)), (has_next, pl.ds(6, 2))):

        @pl.when(jnp.logical_not(there))
        def _():
            base[:, :, at] = jnp.zeros((2, 2, 2, half, width), jnp.float32)
            inbound[:, :, at] = jnp.zeros((2, 2, 2, half, width), jnp.float32)

    for there, side in ((has_above, 0), (has_below, 1)):

        @pl.when(jnp.logical_not(there))
        def _():
            inbound[side] = jnp.zeros(inbound.shape[1:], jnp.float32)

    small[0].wait()
    last = count[0] - 1
    at_row = lax.broadcasted_iota(jnp.int32, (planes, planes), 0)
    at_column = lax.broadcasted_iota(jnp.int32, (planes, planes), 1)
    live = (at_row <= last) & (at_column <= last)
    real = jnp.where(live, matrix[0], 0.0)
    imag = jnp.where(live, matrix[1], 0.0)
    end_re = jnp.sum(jnp.where(at_row == last, real, 0.0), axis=0, keepdims=True)
    end_im = jnp.sum(jnp.where(at_row == last, imag, 0.0), axis=0, keepdims=True)
    whole = jnp.concatenate(
        [
            jnp.concatenate([real, -imag], axis=1),
            jnp.concatenate([imag, real], axis=1),
            jnp.concatenate(
                [
                    jnp.concatenate([end_re, -end_im], axis=1),
                    jnp.concatenate([end_im, end_re], axis=1),
                    jnp.concatenate([real[:1], -imag[:1]], axis=1),
                    jnp.concatenate([imag[:1], real[:1]], axis=1),
                    jnp.zeros((EXTRA - 4, 2 * planes), jnp.float32),
                ],
                axis=0,
            ),
        ],
        axis=0,
    )
    high = whole.astype(jnp.bfloat16)
    low = (whole - high.astype(jnp.float32)).astype(jnp.bfloat16)
    tall = 2 * planes + EXTRA
    weights[:tall] = high
    weights[tall:] = low
    for side, pick in ((0, at_column == 0), (1, at_column == last)):
        for part, values in ((0, real), (1, imag)):
            picked = jnp.sum(jnp.where(pick, values, 0.0), axis=1, keepdims=True)
            column[side, part] = jnp.broadcast_to(picked, (planes, 128))
    for part, values in ((0, real), (1, imag)):
        for side, pick in ((0, (at_row == last) & (at_column == 0)), (1, (at_row == 0) & (at_column == last))):
            picked = jnp.sum(jnp.sum(jnp.where(pick, values, 0.0), axis=1, keepdims=True), axis=0, keepdims=True)
            coeff[side, part] = jnp.broadcast_to(picked, (half, 128))

    def solve(s, r):
        load(s, r).wait()
        values = held[s, r].reshape(2 * planes, width)
        upper = values.astype(jnp.bfloat16)
        lower = (values - upper.astype(jnp.float32)).astype(jnp.bfloat16)
        first = jnp.dot(weights[...], upper, preferred_element_type=jnp.float32)
        second = jnp.dot(weights[:tall], lower, preferred_element_type=jnp.float32)
        total = first[:tall] + first[tall:] + second
        solved[s, r] = total[: 2 * planes].reshape(2, planes, width)
        side = s // half
        for part in range(2):
            row = jnp.where(
                side == 0,
                total[2 * planes + part : 2 * planes + part + 1],
                total[2 * planes + 2 + part : 2 * planes + 3 + part],
            )
            base[side, part, r + 2, pl.ds(s % half, 1), :] = row

    cut = planes - RELAY

    def piece(k, to_next, stop=planes):
        s, a, count_rows, part, parts = PIECES[k]
        row, at = (rows - a - count_rows, 2 - a - count_rows) if to_next else (a, 2 + a)
        return pltpu.make_async_remote_copy(
            src_ref=solved.at[s, pl.ds(row, count_rows), pl.ds(part, parts), pl.ds(0, stop)],
            dst_ref=halo.at[s, pl.ds(at, count_rows), pl.ds(part, parts), pl.ds(0, stop)],
            send_sem=bulk_send.at[int(to_next), k],
            recv_sem=bulk_recv.at[int(to_next), k],
            device_id=(d, l + 1 if to_next else l - 1),
            device_id_type=MESH,
        )

    relays = (
        (0, 0, (at_pair == 3) | ((at_pair == 7) & has_next), -1),
        (0, 1, (at_pair == 2) | ((at_pair == 6) & (l + 2 < tiles)), jnp.where(at_pair == 6, 7, -1)),
        (0, 2, (at_pair == 1) | ((at_pair == 5) & (l > 5)), jnp.where(at_pair == 5, -5, 3)),
        (1, 0, (at_pair == 4) | ((at_pair == 0) & has_prev), 1),
        (1, 1, (at_pair == 5) | ((at_pair == 1) & (l > 1)), jnp.where(at_pair == 1, -7, 1)),
        (1, 2, (at_pair == 6) | ((at_pair == 2) & (l + 6 < tiles)), jnp.where(at_pair == 2, 5, -3)),
    )
    relay_by = {(way, stage): by for way, stage, _, by in relays}

    def relay(way, stage):
        if stage == 0:
            kept = solved.at[0, 0 if way else rows - 1, 0, pl.ds(cut, RELAY)]
        else:
            kept = passed.at[way, stage - 1]
        there = halo.at[0, 2 if way else 1, 0, pl.ds(cut, RELAY)] if stage == 2 else passed.at[way, stage]
        return pltpu.make_async_remote_copy(
            src_ref=kept,
            dst_ref=there,
            send_sem=relay_send.at[way, stage],
            recv_sem=relay_recv.at[way, stage],
            device_id=(d, l + relay_by[way, stage]),
            device_id_type=MESH,
        )

    def relay_on(stage):
        for way, at, here, _ in relays:
            if at == stage:

                @pl.when(here)
                def _():
                    if stage > 0:
                        relay(way, stage - 1).wait_recv()
                    relay(way, stage).start()

    def send_pieces(start, stop):
        for to_next, there in ((False, has_prev), (True, has_next)):

            @pl.when(there)
            def _():
                for k in range(start, stop):
                    piece(k, to_next).start()

    def send_first(to_next, there, stop):
        @pl.when(there)
        def _():
            piece(0, to_next, stop).start()
            for k in range(1, AFTER_FIRST):
                piece(k, to_next).start()

    solve(0, 0)
    solve(0, 3)

    def tell_layers():
        for there, by_d in ((has_above, -1), (has_below, 1)):

            @pl.when(there)
            def _():
                pl.semaphore_signal(ready_sem, inc=1, device_id=(d + by_d, l), device_id_type=MESH)

    @pl.when(jnp.logical_not(seam))
    def _():
        pl.semaphore_wait(barrier, tiles_beside + tiles_beyond + layers_beside)
        for there, by_l in ((has_prev & seam_at(l - 1), -1), (has_next & seam_at(l + 1), 1)):

            @pl.when(there)
            def _():
                pl.semaphore_signal(near_sem, inc=1, device_id=(d, l + by_l), device_id_type=MESH)

    @pl.when(seam)
    def _():
        pl.semaphore_wait(near_sem, 1)

    near_prev = has_prev & jnp.logical_not(seam_prev)
    near_next = has_next & jnp.logical_not(seam_next)
    send_first(False, near_prev, planes)
    send_first(True, near_next, planes)

    @pl.when(jnp.logical_not(seam))
    def _():
        tell_layers()

    @pl.when(seam)
    def _():
        pl.semaphore_wait(barrier, 1)

    send_first(False, seam_prev, cut)
    send_first(True, seam_next, cut)
    relay_on(0)
    solve(0, 1)
    solve(0, 2)
    send_pieces(AFTER_FIRST, AFTER_SHOT)

    def solve_shot(s, carry):
        for r in range(rows):
            solve(s, r)
        return carry

    lax.fori_loop(1, shots, solve_shot, 0)

    def base_copy(side, to_next):
        source_at, target_at = (4, 0) if to_next else (2, 6)
        return pltpu.make_async_remote_copy(
            src_ref=base.at[side, :, pl.ds(source_at, 2)],
            dst_ref=base.at[side, :, pl.ds(target_at, 2)],
            send_sem=base_send.at[int(to_next), side],
            recv_sem=base_recv.at[int(to_next), side],
            device_id=(d, l + 1 if to_next else l - 1),
            device_id_type=MESH,
        )

    base_copies = tuple(
        (needed, to_next, side)
        for needed, side in ((True, side_one), (inner, side_two))
        for to_next in (False, True)
    )

    def both(needed, there):
        return there if needed is True else needed & there

    @pl.when(jnp.logical_not(seam))
    def _():
        pl.semaphore_wait(ready_sem, layers_beside)

    for needed, to_next, side in base_copies:

        @pl.when(both(needed, has_next if to_next else has_prev))
        def _():
            base_copy(side, to_next).start()

    @pl.when(inner)
    def _():
        send_pieces(AFTER_SHOT, AFTER_BASE_INNER)

    @pl.when(jnp.logical_not(inner))
    def _():
        send_pieces(AFTER_SHOT, AFTER_BASE_OUTER)

    small[1].wait()
    small[2].wait()
    for r in range(rows):
        load_cells(r).wait()

        def look_up(i, carry):
            at = pl.ds(pl.multiple_of(i * BLOCK, BLOCK), BLOCK)
            kinds = cells[r, at, :]
            re = jnp.full(kinds.shape, table_re[0], jnp.float32)
            im = jnp.full(kinds.shape, table_im[0], jnp.float32)
            for kind in range(1, CLASSES):
                hit = kinds == kind
                re = jnp.where(hit, table_re[kind], re)
                im = jnp.where(hit, table_im[kind], im)
            kappa[r, 0, at, :] = re
            kappa[r, 1, at, :] = im
            bottom = lax.broadcasted_iota(jnp.int32, kinds.shape, 0) + i * BLOCK == last
            return (carry[0] + jnp.where(bottom, re, 0.0), carry[1] + jnp.where(bottom, im, 0.0))

        zeros = jnp.zeros((BLOCK, width), jnp.float32)
        sums = lax.fori_loop(0, planes // BLOCK, look_up, (zeros, zeros))
        for part in range(2):
            plane[0, part, r] = jnp.broadcast_to(jnp.sum(sums[part], axis=0, keepdims=True), (half, width))
            plane[1, part, r] = jnp.broadcast_to(kappa[r, part, pl.ds(0, 1), :], (half, width))

    for needed, to_next, side in base_copies:

        @pl.when(both(needed, has_prev if to_next else has_next))
        def _():
            base_copy(side, to_next).wait_recv()

    @pl.when(seam)
    def _():
        tell_layers()
        pl.semaphore_wait(ready_sem, layers_beside)

    relay_on(1)

    def lateral(values, r):
        at = r + 2
        return (
            NEAR * (values[at - 1] + values[at + 1])
            + FAR * (values[at - 2] + values[at + 2])
            + along_y(values[at])
            - 5.0 * values[at]
        )

    def trace_copies(side):
        to = d + 1 - 2 * side
        return (
            (
                True,
                True,
                lambda: pltpu.make_async_remote_copy(
                    src_ref=outbound.at[side],
                    dst_ref=inbound.at[side, :, pl.ds(2, 4)],
                    send_sem=trace_send.at[side, 0],
                    recv_sem=trace_recv.at[side, 0],
                    device_id=(to, l),
                    device_id_type=MESH,
                ),
            ),
            (
                has_prev,
                has_next,
                lambda: pltpu.make_async_remote_copy(
                    src_ref=outbound.at[side, :, pl.ds(0, 2)],
                    dst_ref=inbound.at[side, :, pl.ds(6, 2)],
                    send_sem=trace_send.at[side, 1],
                    recv_sem=trace_recv.at[side, 1],
                    device_id=(to, l - 1),
                    device_id_type=MESH,
                ),
            ),
            (
                has_next,
                has_prev,
                lambda: pltpu.make_async_remote_copy(
                    src_ref=outbound.at[side, :, pl.ds(2, 2)],
                    dst_ref=inbound.at[side, :, pl.ds(0, 2)],
                    send_sem=trace_send.at[side, 2],
                    recv_sem=trace_recv.at[side, 2],
                    device_id=(to, l + 1),
                    device_id_type=MESH,
                ),
            ),
        )

    def under(there, act):
        if there is True:
            act()
        else:
            pl.when(there)(act)

    def emit(side):
        factor = [
            jnp.concatenate([coeff[side, part]] * (width // 128), axis=1) for part in range(2)
        ]
        planar = ([], [])
        for row in range(rows + 4):
            t_re, t_im = inbound[side, 0, row], inbound[side, 1, row]
            planar[0].append(base[side, 0, row] + factor[0] * t_re - factor[1] * t_im)
            planar[1].append(base[side, 1, row] + factor[0] * t_im + factor[1] * t_re)
        for r in range(rows):
            re, im = planar[0][r + 2], planar[1][r + 2]
            k_re, k_im = plane[side, 0, r], plane[side, 1, r]
            outbound[side, 0, r] = re + CORRECTION * (lateral(planar[0], r) + k_re * re - k_im * im)
            outbound[side, 1, r] = im + CORRECTION * (lateral(planar[1], r) + k_re * im + k_im * re)
        for goes, _, copy in trace_copies(side):
            under(goes, lambda: copy().start())

    def take(side):
        for _, comes, copy in trace_copies(side):
            under(comes, lambda: copy().wait_recv())

    @pl.when(inner)
    def _():
        take(side_one)

    emit(side_one)

    @pl.when(inner)
    def _():
        send_pieces(AFTER_BASE_INNER, AFTER_TRACE_INNER)

    @pl.when(jnp.logical_not(inner))
    def _():
        send_pieces(AFTER_BASE_OUTER, AFTER_TRACE_OUTER)

    take(side_two)

    @pl.when(inner)
    def _():
        emit(side_two)

    relay_on(2)

    @pl.when(inner)
    def _():
        send_pieces(AFTER_TRACE_INNER, len(PIECES))

    @pl.when(jnp.logical_not(inner))
    def _():
        send_pieces(AFTER_TRACE_OUTER, len(PIECES))

    for side in range(2):
        for part in range(2):
            values = [inbound[side, part, row] for row in range(rows + 4)]
            for r in range(rows):
                spread[side, part, r] = values[r + 2] + CORRECTION * lateral(values, r)

    def own_rows(s, carry):
        side, shot = s // half, s % half
        for r in range(rows):
            t = [inbound[side, part, r + 2, pl.ds(shot, 1), :] for part in range(2)]
            e = [spread[side, part, r, pl.ds(shot, 1), :] for part in range(2)]

            def block(i, inside):
                at = pl.ds(pl.multiple_of(i * BLOCK, BLOCK), BLOCK)
                g_re, g_im = (
                    jnp.concatenate([column[side, part, at, :]] * (width // 128), axis=1) for part in range(2)
                )
                linear, values = [], []
                for part in range(2):
                    v = solved[s, r, part, at, :]
                    near = [solved[s, q, part, at, :] for q in (r - 1, r + 1) if 0 <= q < rows]
                    far = [solved[s, q, part, at, :] for q in (r - 2, r + 2) if 0 <= q < rows]
                    total = along_y(v) - 5.0 * v + NEAR * sum(near[1:], near[0]) + FAR * sum(far[1:], far[0])
                    linear.append(v + CORRECTION * total)
                    values.append(v)
                v_re = values[0] + g_re * t[0] - g_im * t[1]
                v_im = values[1] + g_re * t[1] + g_im * t[0]
                k_re, k_im = kappa[r, 0, at, :], kappa[r, 1, at, :]
                field[s, r, 0, at, :] = (
                    linear[0] + g_re * e[0] - g_im * e[1] + CORRECTION * (k_re * v_re - k_im * v_im)
                )
                field[s, r, 1, at, :] = (
                    linear[1] + g_re * e[1] + g_im * e[0] + CORRECTION * (k_re * v_im + k_im * v_re)
                )
                return inside

            lax.fori_loop(0, planes // BLOCK, block, 0)
        return carry

    lax.fori_loop(0, shots, own_rows, 0)

    def add_rows(s, part, q, to_rows, start=0, stop=planes):
        for first in range(start, stop, BLOCK):
            at = pl.ds(first, min(BLOCK, stop - first))
            v = halo[s, q, part, at, :]
            for r, weight in to_rows:
                field[s, r, part, at, :] = field[s, r, part, at, :] + (CORRECTION * weight) * v

    for needed, to_next, side in base_copies:

        @pl.when(both(needed, has_next if to_next else has_prev))
        def _():
            base_copy(side, to_next).wait_send()

    for goes, _, copy in trace_copies(side_one):
        under(goes, lambda: copy().wait_send())

    @pl.when(inner)
    def _():
        for goes, _, copy in trace_copies(side_two):
            under(goes, lambda: copy().wait_send())

    from_next = (((3, NEAR), (2, FAR)), ((3, FAR),))
    from_prev = (((0, NEAR), (1, FAR)), ((0, FAR),))

    def add_piece(k, to_next, there, stop=planes):
        s, first_row, count_rows, first_part, parts = PIECES[k]

        @pl.when(there)
        def _():
            piece(k, not to_next, stop).wait_recv()
            piece(k, to_next, stop).wait_send()
            for a in range(first_row, first_row + count_rows):
                q, to_rows = (2 + a, from_next[a]) if to_next else (1 - a, from_prev[a])

                def add_part(part, carry):
                    add_rows(s, part, q, to_rows, 0, stop)
                    return carry

                if parts == 1:
                    add_part(first_part, 0)
                else:
                    lax.fori_loop(first_part, first_part + parts, add_part, 0)

    add_piece(0, True, near_next)
    add_piece(0, False, near_prev)
    add_piece(0, True, seam_next, cut)
    add_piece(0, False, seam_prev, cut)
    for k in range(1, AFTER_TRACE_INNER):
        add_piece(k, True, has_next)
        add_piece(k, False, has_prev)
    for way, stage, here, _ in relays:

        @pl.when(here)
        def _():
            relay(way, stage).wait_send()

    for to_next, there in ((True, seam_next), (False, seam_prev)):

        @pl.when(there)
        def _():
            relay(1 if to_next else 0, 2).wait_recv()
            add_rows(0, 0, 2 if to_next else 1, (from_next if to_next else from_prev)[0], cut, planes)

    for k in range(AFTER_TRACE_INNER, len(PIECES)):
        add_piece(k, True, has_next)
        add_piece(k, False, has_prev)


def write_kernel(field, out, sem):
    shots, rows = field.shape[:2]

    def copy(s, r):
        return pltpu.make_async_copy(field.at[s, r], out.at[s, :, :, r, :], sem.at[s, r])

    for s in range(shots):
        for r in range(rows):
            copy(s, r).start()
    for s in range(shots):
        for r in range(rows):
            copy(s, r).wait()


def on_device(source, line_inverse, plane_count, classes, table_re, table_im):
    shots, parts, planes, rows, width = source.shape
    half = shots // 2
    by_rows = (shots, rows, parts, planes, width)
    any_space = pl.BlockSpec(memory_space=pl.ANY)
    hbm = pl.BlockSpec(memory_space=pltpu.HBM)
    vmem = pl.BlockSpec(memory_space=pltpu.VMEM)
    tall = 2 * planes + EXTRA
    pieces = len(PIECES)
    dma = pltpu.SemaphoreType.DMA
    operands = (source, line_inverse, classes, table_re, table_im)
    field = pl.pallas_call(
        field_kernel,
        out_shape=jax.ShapeDtypeStruct(by_rows, jnp.float32),
        in_specs=[pl.BlockSpec(memory_space=pltpu.SMEM)] + [hbm] * len(operands),
        out_specs=vmem,
        scratch_shapes=[
            pltpu.VMEM((parts, planes, planes), jnp.float32),
            pltpu.SMEM((CLASSES,), jnp.float32),
            pltpu.SMEM((CLASSES,), jnp.float32),
            pltpu.VMEM(by_rows, jnp.float32),
            pltpu.VMEM((rows, planes, width), jnp.int32),
            pltpu.VMEM(by_rows, jnp.float32),
            pltpu.VMEM((shots, 4, parts, planes, width), jnp.float32),
            pltpu.VMEM((rows, parts, planes, width), jnp.float32),
            pltpu.VMEM((2, parts, rows, half, width), jnp.float32),
            pltpu.VMEM((2, parts, rows + 4, half, width), jnp.float32),
            pltpu.VMEM((2, parts, rows + 4, half, width), jnp.float32),
            pltpu.VMEM((2, parts, rows, half, width), jnp.float32),
            pltpu.VMEM((2, parts, rows, half, width), jnp.float32),
            pltpu.VMEM((2, parts, planes, 128), jnp.float32),
            pltpu.VMEM((2, parts, half, 128), jnp.float32),
            pltpu.VMEM((2 * tall, 2 * planes), jnp.bfloat16),
            dma((3,)),
            dma((shots, rows)),
            dma((rows,)),
            dma((2, pieces)),
            dma((2, pieces)),
            dma((2, 2)),
            dma((2, 2)),
            dma((2, 3)),
            dma((2, 3)),
            pltpu.SemaphoreType.REGULAR,
            pltpu.SemaphoreType.REGULAR,
            dma((2, 3)),
            dma((2, 3)),
            pltpu.VMEM((2, 2, RELAY, width), jnp.float32),
        ],
        compiler_params=pltpu.CompilerParams(
            collective_id=0, has_side_effects=True, vmem_limit_bytes=40 * 2**20
        ),
    )(plane_count, *(pltpu.with_memory_space_constraint(x, pltpu.HBM) for x in operands))
    return pl.pallas_call(
        write_kernel,
        out_shape=jax.ShapeDtypeStruct(source.shape, jnp.float32),
        in_specs=[vmem],
        out_specs=any_space,
        scratch_shapes=[dma((shots, rows))],
        compiler_params=pltpu.CompilerParams(vmem_limit_bytes=8 * 2**20),
    )(field)


def solution(mesh):
    in_specs = (
        P(None, None, "depth", "lat", None),
        P("depth", None, None, None),
        P("depth"),
        P("depth", "lat", None),
        P(),
        P(),
    )
    out_specs = P(None, None, "depth", "lat", None)
    return jax.shard_map(
        on_device, mesh=mesh, in_specs=in_specs, out_specs=out_specs, check_vma=False
    )
```

```python
import functools

import jax
import jax.numpy as jnp
from jax import lax
from jax.experimental import pallas as pl
from jax.experimental.pallas import tpu as pltpu
from jax.sharding import PartitionSpec as P

MESH = pl.DeviceIdType.MESH
CLASSES = 16
CORRECTION = 0.1
NEAR = 4.0 / 3.0
FAR = -1.0 / 12.0
BLOCK = 16
EXTRA = 16
RING = 4
RELAY = 48
PIECES = (
    (0, 0, 1, 0, 1),
    (0, 0, 1, 1, 1),
    (0, 1, 1, 0, 2),
    (1, 0, 2, 0, 2),
    (2, 0, 2, 0, 2),
    (3, 0, 1, 0, 2),
    (3, 1, 1, 0, 1),
    (3, 1, 1, 1, 1),
)
AFTER_FIRST = 2
AFTER_SHOT = 3
AFTER_BASE_OUTER = 3
AFTER_BASE_INNER = 4
AFTER_TRACE_INNER = 4
AFTER_TRACE_OUTER = 6


def along_y(x):
    size = x.shape[1]
    lane = lax.broadcasted_iota(jnp.int32, x.shape, 1)
    near = jnp.where(lane >= 1, pltpu.roll(x, 1, 1), 0.0) + jnp.where(
        lane < size - 1, pltpu.roll(x, size - 1, 1), 0.0
    )
    far = jnp.where(lane >= 2, pltpu.roll(x, 2, 1), 0.0) + jnp.where(
        lane < size - 2, pltpu.roll(x, size - 2, 1), 0.0
    )
    return NEAR * near + FAR * far


def field_kernel(
    count, source, matrix_from, classes, table_re_from, table_im_from, field,
    matrix, table_re, table_im,
    held, cells, solved, halo, kappa, plane, base, inbound, outbound, spread, column, coeff, weights,
    small_sem, load_sem, cell_sem, bulk_send, bulk_recv, base_send, base_recv, trace_send, trace_recv,
    ready_sem, near_sem, relay_send, relay_recv, passed,
):
    shots, rows, _, planes, width = held.shape
    half = shots // 2
    d = lax.axis_index("depth")
    l = lax.axis_index("lat")
    layers = lax.axis_size("depth")
    tiles = lax.axis_size("lat")
    has_prev = l > 0
    has_next = l < tiles - 1
    has_above = d > 0
    has_below = d < layers - 1
    inner = has_above & has_below
    seam_prev = has_prev & (l % RING == 0)
    seam_next = has_next & (l % RING == RING - 1)
    seam = seam_prev | seam_next
    at_pair = l % (2 * RING)

    def seam_at(tile):
        at = tile % RING
        return ((tile > 0) & (at == 0)) | ((tile < tiles - 1) & (at == RING - 1))

    side_one = jnp.where(d >= layers // 2, 1, 0)
    side_two = 1 - side_one

    def load(s, r):
        return pltpu.make_async_copy(source.at[s, :, :, r, :], held.at[s, r], load_sem.at[s, r])

    def load_cells(r):
        return pltpu.make_async_copy(classes.at[:, r, :], cells.at[r], cell_sem.at[r])

    small = [
        pltpu.make_async_copy(here, there, small_sem.at[i])
        for i, (here, there) in enumerate(
            ((matrix_from.at[0], matrix), (table_re_from, table_re), (table_im_from, table_im))
        )
    ]
    barrier = pltpu.get_barrier_semaphore()
    for there, by_d, by_l in (
        (has_prev & (seam | jnp.logical_not(seam_at(l - 1))), 0, -1),
        (has_next & (seam | jnp.logical_not(seam_at(l + 1))), 0, 1),
        (has_above & jnp.logical_not(seam), -1, 0),
        (has_below & jnp.logical_not(seam), 1, 0),
        ((at_pair == 5) & (l > 5), 0, -7),
        ((at_pair == 2) & (l + 6 < tiles), 0, 7),
    ):

        @pl.when(there)
        def _():
            pl.semaphore_signal(barrier, inc=1, device_id=(d + by_d, l + by_l), device_id_type=MESH)

    layers_beside = jnp.where(has_above, 1, 0) + jnp.where(has_below, 1, 0)
    tiles_beside = jnp.where(has_prev, 1, 0) + jnp.where(has_next, 1, 0)
    tiles_beyond = jnp.where(((at_pair == 6) & (l + 2 < tiles)) | ((at_pair == 1) & (l > 1)), 1, 0)

    small[0].start()
    for r in (0, 3, 1, 2):
        load(0, r).start()
    small[1].start()
    small[2].start()
    for s in range(1, shots):
        for r in range(rows):
            load(s, r).start()
    for r in range(rows):
        load_cells(r).start()

    for there, at in ((has_prev, pl.ds(0, 2)), (has_next, pl.ds(6, 2))):

        @pl.when(jnp.logical_not(there))
        def _():
            base[:, :, at] = jnp.zeros((2, 2, 2, half, width), jnp.float32)
            inbound[:, :, at] = jnp.zeros((2, 2, 2, half, width), jnp.float32)

    for there, side in ((has_above, 0), (has_below, 1)):

        @pl.when(jnp.logical_not(there))
        def _():
            inbound[side] = jnp.zeros(inbound.shape[1:], jnp.float32)

    small[0].wait()
    last = count[0] - 1
    at_row = lax.broadcasted_iota(jnp.int32, (planes, planes), 0)
    at_column = lax.broadcasted_iota(jnp.int32, (planes, planes), 1)
    live = (at_row <= last) & (at_column <= last)
    real = jnp.where(live, matrix[0], 0.0)
    imag = jnp.where(live, matrix[1], 0.0)
    end_re = jnp.sum(jnp.where(at_row == last, real, 0.0), axis=0, keepdims=True)
    end_im = jnp.sum(jnp.where(at_row == last, imag, 0.0), axis=0, keepdims=True)
    whole = jnp.concatenate(
        [
            jnp.concatenate([real, -imag], axis=1),
            jnp.concatenate([imag, real], axis=1),
            jnp.concatenate(
                [
                    jnp.concatenate([end_re, -end_im], axis=1),
                    jnp.concatenate([end_im, end_re], axis=1),
                    jnp.concatenate([real[:1], -imag[:1]], axis=1),
                    jnp.concatenate([imag[:1], real[:1]], axis=1),
                    jnp.zeros((EXTRA - 4, 2 * planes), jnp.float32),
                ],
                axis=0,
            ),
        ],
        axis=0,
    )
    high = whole.astype(jnp.bfloat16)
    low = (whole - high.astype(jnp.float32)).astype(jnp.bfloat16)
    tall = 2 * planes + EXTRA
    weights[:tall] = high
    weights[tall:] = low
    for side, pick in ((0, at_column == 0), (1, at_column == last)):
        for part, values in ((0, real), (1, imag)):
            picked = jnp.sum(jnp.where(pick, values, 0.0), axis=1, keepdims=True)
            column[side, part] = jnp.broadcast_to(picked, (planes, 128))
    for part, values in ((0, real), (1, imag)):
        for side, pick in ((0, (at_row == last) & (at_column == 0)), (1, (at_row == 0) & (at_column == last))):
            picked = jnp.sum(jnp.sum(jnp.where(pick, values, 0.0), axis=1, keepdims=True), axis=0, keepdims=True)
            coeff[side, part] = jnp.broadcast_to(picked, (half, 128))

    def solve(s, r):
        load(s, r).wait()
        values = held[s, r].reshape(2 * planes, width)
        upper = values.astype(jnp.bfloat16)
        lower = (values - upper.astype(jnp.float32)).astype(jnp.bfloat16)
        first = jnp.dot(weights[...], upper, preferred_element_type=jnp.float32)
        second = jnp.dot(weights[:tall], lower, preferred_element_type=jnp.float32)
        total = first[:tall] + first[tall:] + second
        solved[s, r] = total[: 2 * planes].reshape(2, planes, width)
        side = s // half
        for part in range(2):
            row = jnp.where(
                side == 0,
                total[2 * planes + part : 2 * planes + part + 1],
                total[2 * planes + 2 + part : 2 * planes + 3 + part],
            )
            base[side, part, r + 2, pl.ds(s % half, 1), :] = row

    cut = planes - RELAY

    def piece(k, to_next, stop=planes):
        s, a, count_rows, part, parts = PIECES[k]
        row, at = (rows - a - count_rows, 2 - a - count_rows) if to_next else (a, 2 + a)
        return pltpu.make_async_remote_copy(
            src_ref=solved.at[s, pl.ds(row, count_rows), pl.ds(part, parts), pl.ds(0, stop)],
            dst_ref=halo.at[s, pl.ds(at, count_rows), pl.ds(part, parts), pl.ds(0, stop)],
            send_sem=bulk_send.at[int(to_next), k],
            recv_sem=bulk_recv.at[int(to_next), k],
            device_id=(d, l + 1 if to_next else l - 1),
            device_id_type=MESH,
        )

    relays = (
        (0, 0, (at_pair == 3) | ((at_pair == 7) & has_next), -1),
        (0, 1, (at_pair == 2) | ((at_pair == 6) & (l + 2 < tiles)), jnp.where(at_pair == 6, 7, -1)),
        (0, 2, (at_pair == 1) | ((at_pair == 5) & (l > 5)), jnp.where(at_pair == 5, -5, 3)),
        (1, 0, (at_pair == 4) | ((at_pair == 0) & has_prev), 1),
        (1, 1, (at_pair == 5) | ((at_pair == 1) & (l > 1)), jnp.where(at_pair == 1, -7, 1)),
        (1, 2, (at_pair == 6) | ((at_pair == 2) & (l + 6 < tiles)), jnp.where(at_pair == 2, 5, -3)),
    )
    relay_by = {(way, stage): by for way, stage, _, by in relays}

    def relay(way, stage):
        if stage == 0:
            kept = solved.at[0, 0 if way else rows - 1, 0, pl.ds(cut, RELAY)]
        else:
            kept = passed.at[way, stage - 1]
        there = halo.at[0, 2 if way else 1, 0, pl.ds(cut, RELAY)] if stage == 2 else passed.at[way, stage]
        return pltpu.make_async_remote_copy(
            src_ref=kept,
            dst_ref=there,
            send_sem=relay_send.at[way, stage],
            recv_sem=relay_recv.at[way, stage],
            device_id=(d, l + relay_by[way, stage]),
            device_id_type=MESH,
        )

    def relay_on(stage):
        for way, at, here, _ in relays:
            if at == stage:

                @pl.when(here)
                def _():
                    if stage > 0:
                        relay(way, stage - 1).wait_recv()
                    relay(way, stage).start()

    def send_pieces(start, stop):
        for to_next, there in ((False, has_prev), (True, has_next)):

            @pl.when(there)
            def _():
                for k in range(start, stop):
                    piece(k, to_next).start()

    def send_first(to_next, there, stop):
        @pl.when(there)
        def _():
            piece(0, to_next, stop).start()
            for k in range(1, AFTER_FIRST):
                piece(k, to_next).start()

    solve(0, 0)
    solve(0, 3)

    def tell_layers():
        for there, by_d in ((has_above, -1), (has_below, 1)):

            @pl.when(there)
            def _():
                pl.semaphore_signal(ready_sem, inc=1, device_id=(d + by_d, l), device_id_type=MESH)

    @pl.when(jnp.logical_not(seam))
    def _():
        pl.semaphore_wait(barrier, tiles_beside + tiles_beyond + layers_beside)
        for there, by_l in ((has_prev & seam_at(l - 1), -1), (has_next & seam_at(l + 1), 1)):

            @pl.when(there)
            def _():
                pl.semaphore_signal(near_sem, inc=1, device_id=(d, l + by_l), device_id_type=MESH)

    @pl.when(seam)
    def _():
        pl.semaphore_wait(near_sem, 1)

    near_prev = has_prev & jnp.logical_not(seam_prev)
    near_next = has_next & jnp.logical_not(seam_next)
    send_first(False, near_prev, planes)
    send_first(True, near_next, planes)

    @pl.when(jnp.logical_not(seam))
    def _():
        tell_layers()

    @pl.when(seam)
    def _():
        pl.semaphore_wait(barrier, 1)

    send_first(False, seam_prev, cut)
    send_first(True, seam_next, cut)
    relay_on(0)
    solve(0, 1)
    solve(0, 2)
    send_pieces(AFTER_FIRST, AFTER_SHOT)

    def solve_shot(s, carry):
        for r in range(rows):
            solve(s, r)
        return carry

    lax.fori_loop(1, shots, solve_shot, 0)

    def base_copy(side, to_next):
        source_at, target_at = (4, 0) if to_next else (2, 6)
        return pltpu.make_async_remote_copy(
            src_ref=base.at[side, :, pl.ds(source_at, 2)],
            dst_ref=base.at[side, :, pl.ds(target_at, 2)],
            send_sem=base_send.at[int(to_next), side],
            recv_sem=base_recv.at[int(to_next), side],
            device_id=(d, l + 1 if to_next else l - 1),
            device_id_type=MESH,
        )

    base_copies = tuple(
        (needed, to_next, side)
        for needed, side in ((True, side_one), (inner, side_two))
        for to_next in (False, True)
    )

    def both(needed, there):
        return there if needed is True else needed & there

    @pl.when(jnp.logical_not(seam))
    def _():
        pl.semaphore_wait(ready_sem, layers_beside)

    for needed, to_next, side in base_copies:

        @pl.when(both(needed, has_next if to_next else has_prev))
        def _():
            base_copy(side, to_next).start()

    @pl.when(inner)
    def _():
        send_pieces(AFTER_SHOT, AFTER_BASE_INNER)

    @pl.when(jnp.logical_not(inner))
    def _():
        send_pieces(AFTER_SHOT, AFTER_BASE_OUTER)

    small[1].wait()
    small[2].wait()
    for r in range(rows):
        load_cells(r).wait()

        def look_up(i, carry):
            at = pl.ds(pl.multiple_of(i * BLOCK, BLOCK), BLOCK)
            kinds = cells[r, at, :]
            re = jnp.full(kinds.shape, table_re[0], jnp.float32)
            im = jnp.full(kinds.shape, table_im[0], jnp.float32)
            for kind in range(1, CLASSES):
                hit = kinds == kind
                re = jnp.where(hit, table_re[kind], re)
                im = jnp.where(hit, table_im[kind], im)
            kappa[r, 0, at, :] = re
            kappa[r, 1, at, :] = im
            bottom = lax.broadcasted_iota(jnp.int32, kinds.shape, 0) + i * BLOCK == last
            return (carry[0] + jnp.where(bottom, re, 0.0), carry[1] + jnp.where(bottom, im, 0.0))

        zeros = jnp.zeros((BLOCK, width), jnp.float32)
        sums = lax.fori_loop(0, planes // BLOCK, look_up, (zeros, zeros))
        for part in range(2):
            plane[0, part, r] = jnp.broadcast_to(jnp.sum(sums[part], axis=0, keepdims=True), (half, width))
            plane[1, part, r] = jnp.broadcast_to(kappa[r, part, pl.ds(0, 1), :], (half, width))

    for needed, to_next, side in base_copies:

        @pl.when(both(needed, has_prev if to_next else has_next))
        def _():
            base_copy(side, to_next).wait_recv()

    @pl.when(seam)
    def _():
        tell_layers()
        pl.semaphore_wait(ready_sem, layers_beside)

    relay_on(1)

    def lateral(values, r):
        at = r + 2
        return (
            NEAR * (values[at - 1] + values[at + 1])
            + FAR * (values[at - 2] + values[at + 2])
            + along_y(values[at])
            - 5.0 * values[at]
        )

    def trace_copies(side):
        to = d + 1 - 2 * side
        return (
            (
                True,
                True,
                lambda: pltpu.make_async_remote_copy(
                    src_ref=outbound.at[side],
                    dst_ref=inbound.at[side, :, pl.ds(2, 4)],
                    send_sem=trace_send.at[side, 0],
                    recv_sem=trace_recv.at[side, 0],
                    device_id=(to, l),
                    device_id_type=MESH,
                ),
            ),
            (
                has_prev,
                has_next,
                lambda: pltpu.make_async_remote_copy(
                    src_ref=outbound.at[side, :, pl.ds(0, 2)],
                    dst_ref=inbound.at[side, :, pl.ds(6, 2)],
                    send_sem=trace_send.at[side, 1],
                    recv_sem=trace_recv.at[side, 1],
                    device_id=(to, l - 1),
                    device_id_type=MESH,
                ),
            ),
            (
                has_next,
                has_prev,
                lambda: pltpu.make_async_remote_copy(
                    src_ref=outbound.at[side, :, pl.ds(2, 2)],
                    dst_ref=inbound.at[side, :, pl.ds(0, 2)],
                    send_sem=trace_send.at[side, 2],
                    recv_sem=trace_recv.at[side, 2],
                    device_id=(to, l + 1),
                    device_id_type=MESH,
                ),
            ),
        )

    def under(there, act):
        if there is True:
            act()
        else:
            pl.when(there)(act)

    def emit(side):
        factor = [
            jnp.concatenate([coeff[side, part]] * (width // 128), axis=1) for part in range(2)
        ]
        planar = ([], [])
        for row in range(rows + 4):
            t_re, t_im = inbound[side, 0, row], inbound[side, 1, row]
            planar[0].append(base[side, 0, row] + factor[0] * t_re - factor[1] * t_im)
            planar[1].append(base[side, 1, row] + factor[0] * t_im + factor[1] * t_re)
        for r in range(rows):
            re, im = planar[0][r + 2], planar[1][r + 2]
            k_re, k_im = plane[side, 0, r], plane[side, 1, r]
            outbound[side, 0, r] = re + CORRECTION * (lateral(planar[0], r) + k_re * re - k_im * im)
            outbound[side, 1, r] = im + CORRECTION * (lateral(planar[1], r) + k_re * im + k_im * re)
        for goes, _, copy in trace_copies(side):
            under(goes, lambda: copy().start())

    def take(side):
        for _, comes, copy in trace_copies(side):
            under(comes, lambda: copy().wait_recv())

    @pl.when(inner)
    def _():
        take(side_one)

    emit(side_one)

    @pl.when(inner)
    def _():
        send_pieces(AFTER_BASE_INNER, AFTER_TRACE_INNER)

    @pl.when(jnp.logical_not(inner))
    def _():
        send_pieces(AFTER_BASE_OUTER, AFTER_TRACE_OUTER)

    take(side_two)

    @pl.when(inner)
    def _():
        emit(side_two)

    relay_on(2)

    @pl.when(inner)
    def _():
        send_pieces(AFTER_TRACE_INNER, len(PIECES))

    @pl.when(jnp.logical_not(inner))
    def _():
        send_pieces(AFTER_TRACE_OUTER, len(PIECES))

    for side in range(2):
        for part in range(2):
            values = [inbound[side, part, row] for row in range(rows + 4)]
            for r in range(rows):
                spread[side, part, r] = values[r + 2] + CORRECTION * lateral(values, r)

    def own_rows(s, carry):
        side, shot = s // half, s % half
        for r in range(rows):
            t = [inbound[side, part, r + 2, pl.ds(shot, 1), :] for part in range(2)]
            e = [spread[side, part, r, pl.ds(shot, 1), :] for part in range(2)]

            def block(i, inside):
                at = pl.ds(pl.multiple_of(i * BLOCK, BLOCK), BLOCK)
                g_re, g_im = (
                    jnp.concatenate([column[side, part, at, :]] * (width // 128), axis=1) for part in range(2)
                )
                linear, values = [], []
                for part in range(2):
                    v = solved[s, r, part, at, :]
                    near = [solved[s, q, part, at, :] for q in (r - 1, r + 1) if 0 <= q < rows]
                    far = [solved[s, q, part, at, :] for q in (r - 2, r + 2) if 0 <= q < rows]
                    total = along_y(v) - 5.0 * v + NEAR * sum(near[1:], near[0]) + FAR * sum(far[1:], far[0])
                    linear.append(v + CORRECTION * total)
                    values.append(v)
                v_re = values[0] + g_re * t[0] - g_im * t[1]
                v_im = values[1] + g_re * t[1] + g_im * t[0]
                k_re, k_im = kappa[r, 0, at, :], kappa[r, 1, at, :]
                field[s, r, 0, at, :] = (
                    linear[0] + g_re * e[0] - g_im * e[1] + CORRECTION * (k_re * v_re - k_im * v_im)
                )
                field[s, r, 1, at, :] = (
                    linear[1] + g_re * e[1] + g_im * e[0] + CORRECTION * (k_re * v_im + k_im * v_re)
                )
                return inside

            lax.fori_loop(0, planes // BLOCK, block, 0)
        return carry

    lax.fori_loop(0, shots, own_rows, 0)

    def add_rows(s, part, q, to_rows, start=0, stop=planes):
        for first in range(start, stop, BLOCK):
            at = pl.ds(first, min(BLOCK, stop - first))
            v = halo[s, q, part, at, :]
            for r, weight in to_rows:
                field[s, r, part, at, :] = field[s, r, part, at, :] + (CORRECTION * weight) * v

    for needed, to_next, side in base_copies:

        @pl.when(both(needed, has_next if to_next else has_prev))
        def _():
            base_copy(side, to_next).wait_send()

    for goes, _, copy in trace_copies(side_one):
        under(goes, lambda: copy().wait_send())

    @pl.when(inner)
    def _():
        for goes, _, copy in trace_copies(side_two):
            under(goes, lambda: copy().wait_send())

    from_next = (((3, NEAR), (2, FAR)), ((3, FAR),))
    from_prev = (((0, NEAR), (1, FAR)), ((0, FAR),))

    def add_piece(k, to_next, there, stop=planes):
        s, first_row, count_rows, first_part, parts = PIECES[k]

        @pl.when(there)
        def _():
            piece(k, not to_next, stop).wait_recv()
            piece(k, to_next, stop).wait_send()
            for a in range(first_row, first_row + count_rows):
                q, to_rows = (2 + a, from_next[a]) if to_next else (1 - a, from_prev[a])

                def add_part(part, carry):
                    add_rows(s, part, q, to_rows, 0, stop)
                    return carry

                if parts == 1:
                    add_part(first_part, 0)
                else:
                    lax.fori_loop(first_part, first_part + parts, add_part, 0)

    add_piece(0, True, near_next)
    add_piece(0, False, near_prev)
    add_piece(0, True, seam_next, cut)
    add_piece(0, False, seam_prev, cut)
    for k in range(1, AFTER_TRACE_INNER):
        add_piece(k, True, has_next)
        add_piece(k, False, has_prev)
    for way, stage, here, _ in relays:

        @pl.when(here)
        def _():
            relay(way, stage).wait_send()

    for to_next, there in ((True, seam_next), (False, seam_prev)):

        @pl.when(there)
        def _():
            relay(1 if to_next else 0, 2).wait_recv()
            add_rows(0, 0, 2 if to_next else 1, (from_next if to_next else from_prev)[0], cut, planes)

    for k in range(AFTER_TRACE_INNER, len(PIECES)):
        add_piece(k, True, has_next)
        add_piece(k, False, has_prev)


def write_kernel(field, out, sem):
    shots, rows = field.shape[:2]

    def copy(s, r):
        return pltpu.make_async_copy(field.at[s, r], out.at[s, :, :, r, :], sem.at[s, r])

    for s in range(shots):
        for r in range(rows):
            copy(s, r).start()
    for s in range(shots):
        for r in range(rows):
            copy(s, r).wait()


def on_device(source, line_inverse, plane_count, classes, table_re, table_im):
    shots, parts, planes, rows, width = source.shape
    half = shots // 2
    by_rows = (shots, rows, parts, planes, width)
    any_space = pl.BlockSpec(memory_space=pl.ANY)
    hbm = pl.BlockSpec(memory_space=pltpu.HBM)
    vmem = pl.BlockSpec(memory_space=pltpu.VMEM)
    tall = 2 * planes + EXTRA
    pieces = len(PIECES)
    dma = pltpu.SemaphoreType.DMA
    operands = (source, line_inverse, classes, table_re, table_im)
    field = pl.pallas_call(
        field_kernel,
        out_shape=jax.ShapeDtypeStruct(by_rows, jnp.float32),
        in_specs=[pl.BlockSpec(memory_space=pltpu.SMEM)] + [hbm] * len(operands),
        out_specs=vmem,
        scratch_shapes=[
            pltpu.VMEM((parts, planes, planes), jnp.float32),
            pltpu.SMEM((CLASSES,), jnp.float32),
            pltpu.SMEM((CLASSES,), jnp.float32),
            pltpu.VMEM(by_rows, jnp.float32),
            pltpu.VMEM((rows, planes, width), jnp.int32),
            pltpu.VMEM(by_rows, jnp.float32),
            pltpu.VMEM((shots, 4, parts, planes, width), jnp.float32),
            pltpu.VMEM((rows, parts, planes, width), jnp.float32),
            pltpu.VMEM((2, parts, rows, half, width), jnp.float32),
            pltpu.VMEM((2, parts, rows + 4, half, width), jnp.float32),
            pltpu.VMEM((2, parts, rows + 4, half, width), jnp.float32),
            pltpu.VMEM((2, parts, rows, half, width), jnp.float32),
            pltpu.VMEM((2, parts, rows, half, width), jnp.float32),
            pltpu.VMEM((2, parts, planes, 128), jnp.float32),
            pltpu.VMEM((2, parts, half, 128), jnp.float32),
            pltpu.VMEM((2 * tall, 2 * planes), jnp.bfloat16),
            dma((3,)),
            dma((shots, rows)),
            dma((rows,)),
            dma((2, pieces)),
            dma((2, pieces)),
            dma((2, 2)),
            dma((2, 2)),
            dma((2, 3)),
            dma((2, 3)),
            pltpu.SemaphoreType.REGULAR,
            pltpu.SemaphoreType.REGULAR,
            dma((2, 3)),
            dma((2, 3)),
            pltpu.VMEM((2, 2, RELAY, width), jnp.float32),
        ],
        compiler_params=pltpu.CompilerParams(
            collective_id=0, has_side_effects=True, vmem_limit_bytes=40 * 2**20
        ),
    )(plane_count, *(pltpu.with_memory_space_constraint(x, pltpu.HBM) for x in operands))
    return pl.pallas_call(
        write_kernel,
        out_shape=jax.ShapeDtypeStruct(source.shape, jnp.float32),
        in_specs=[vmem],
        out_specs=any_space,
        scratch_shapes=[dma((shots, rows))],
        compiler_params=pltpu.CompilerParams(vmem_limit_bytes=8 * 2**20),
    )(field)


def solution(mesh):
    in_specs = (
        P(None, None, "depth", "lat", None),
        P("depth", None, None, None),
        P("depth"),
        P("depth", "lat", None),
        P(),
        P(),
    )
    out_specs = P(None, None, "depth", "lat", None)
    return jax.shard_map(
        on_device, mesh=mesh, in_specs=in_specs, out_specs=out_specs, check_vma=False
    )
```

```python
import functools

import jax
import jax.numpy as jnp
from jax import lax
from jax.experimental import pallas as pl
from jax.experimental.pallas import tpu as pltpu
from jax.sharding import PartitionSpec as P

MESH = pl.DeviceIdType.MESH
CLASSES = 16
CORRECTION = 0.1
NEAR = 4.0 / 3.0
FAR = -1.0 / 12.0
BLOCK = 16
EXTRA = 16
RING = 4
RELAY = 48
PIECES = (
    (0, 0, 1, 0, 1),
    (0, 0, 1, 1, 1),
    (0, 1, 1, 0, 2),
    (1, 0, 2, 0, 2),
    (2, 0, 2, 0, 2),
    (3, 0, 1, 0, 2),
    (3, 1, 1, 0, 2),
)
AFTER_FIRST = 2
AFTER_SHOT = 3
AFTER_BASE_OUTER = 3
AFTER_BASE_INNER = 4
AFTER_TRACE_INNER = 4
AFTER_TRACE_OUTER = 6


def along_y(x):
    size = x.shape[1]
    lane = lax.broadcasted_iota(jnp.int32, x.shape, 1)
    near = jnp.where(lane >= 1, pltpu.roll(x, 1, 1), 0.0) + jnp.where(
        lane < size - 1, pltpu.roll(x, size - 1, 1), 0.0
    )
    far = jnp.where(lane >= 2, pltpu.roll(x, 2, 1), 0.0) + jnp.where(
        lane < size - 2, pltpu.roll(x, size - 2, 1), 0.0
    )
    return NEAR * near + FAR * far


def field_kernel(
    count, source, matrix_from, classes, table_re_from, table_im_from, field,
    matrix, table_re, table_im,
    held, cells, solved, halo, kappa, plane, base, inbound, outbound, spread, column, coeff, weights,
    small_sem, load_sem, cell_sem, bulk_send, bulk_recv, base_send, base_recv, trace_send, trace_recv,
    ready_sem, near_sem, relay_send, relay_recv, passed,
):
    shots, rows, _, planes, width = held.shape
    half = shots // 2
    d = lax.axis_index("depth")
    l = lax.axis_index("lat")
    layers = lax.axis_size("depth")
    tiles = lax.axis_size("lat")
    has_prev = l > 0
    has_next = l < tiles - 1
    has_above = d > 0
    has_below = d < layers - 1
    inner = has_above & has_below
    seam_prev = has_prev & (l % RING == 0)
    seam_next = has_next & (l % RING == RING - 1)
    seam = seam_prev | seam_next
    at_pair = l % (2 * RING)

    def seam_at(tile):
        at = tile % RING
        return ((tile > 0) & (at == 0)) | ((tile < tiles - 1) & (at == RING - 1))

    side_one = jnp.where(d >= layers // 2, 1, 0)
    side_two = 1 - side_one

    def load(s, r):
        return pltpu.make_async_copy(source.at[s, :, :, r, :], held.at[s, r], load_sem.at[s, r])

    def load_cells(r):
        return pltpu.make_async_copy(classes.at[:, r, :], cells.at[r], cell_sem.at[r])

    small = [
        pltpu.make_async_copy(here, there, small_sem.at[i])
        for i, (here, there) in enumerate(
            ((matrix_from.at[0], matrix), (table_re_from, table_re), (table_im_from, table_im))
        )
    ]
    barrier = pltpu.get_barrier_semaphore()
    for there, by_d, by_l in (
        (has_prev & (seam | jnp.logical_not(seam_at(l - 1))), 0, -1),
        (has_next & (seam | jnp.logical_not(seam_at(l + 1))), 0, 1),
        (has_above & jnp.logical_not(seam), -1, 0),
        (has_below & jnp.logical_not(seam), 1, 0),
        ((at_pair == 5) & (l > 5), 0, -7),
        ((at_pair == 2) & (l + 6 < tiles), 0, 7),
    ):

        @pl.when(there)
        def _():
            pl.semaphore_signal(barrier, inc=1, device_id=(d + by_d, l + by_l), device_id_type=MESH)

    layers_beside = jnp.where(has_above, 1, 0) + jnp.where(has_below, 1, 0)
    tiles_beside = jnp.where(has_prev, 1, 0) + jnp.where(has_next, 1, 0)
    tiles_beyond = jnp.where(((at_pair == 6) & (l + 2 < tiles)) | ((at_pair == 1) & (l > 1)), 1, 0)

    small[0].start()
    for r in (0, 3, 1, 2):
        load(0, r).start()
    small[1].start()
    small[2].start()
    for s in range(1, shots):
        for r in range(rows):
            load(s, r).start()
    for r in range(rows):
        load_cells(r).start()

    for there, at in ((has_prev, pl.ds(0, 2)), (has_next, pl.ds(6, 2))):

        @pl.when(jnp.logical_not(there))
        def _():
            base[:, :, at] = jnp.zeros((2, 2, 2, half, width), jnp.float32)
            inbound[:, :, at] = jnp.zeros((2, 2, 2, half, width), jnp.float32)

    for there, side in ((has_above, 0), (has_below, 1)):

        @pl.when(jnp.logical_not(there))
        def _():
            inbound[side] = jnp.zeros(inbound.shape[1:], jnp.float32)

    small[0].wait()
    last = count[0] - 1
    at_row = lax.broadcasted_iota(jnp.int32, (planes, planes), 0)
    at_column = lax.broadcasted_iota(jnp.int32, (planes, planes), 1)
    live = (at_row <= last) & (at_column <= last)
    real = jnp.where(live, matrix[0], 0.0)
    imag = jnp.where(live, matrix[1], 0.0)
    end_re = jnp.sum(jnp.where(at_row == last, real, 0.0), axis=0, keepdims=True)
    end_im = jnp.sum(jnp.where(at_row == last, imag, 0.0), axis=0, keepdims=True)
    whole = jnp.concatenate(
        [
            jnp.concatenate([real, -imag], axis=1),
            jnp.concatenate([imag, real], axis=1),
            jnp.concatenate(
                [
                    jnp.concatenate([end_re, -end_im], axis=1),
                    jnp.concatenate([end_im, end_re], axis=1),
                    jnp.concatenate([real[:1], -imag[:1]], axis=1),
                    jnp.concatenate([imag[:1], real[:1]], axis=1),
                    jnp.zeros((EXTRA - 4, 2 * planes), jnp.float32),
                ],
                axis=0,
            ),
        ],
        axis=0,
    )
    high = whole.astype(jnp.bfloat16)
    low = (whole - high.astype(jnp.float32)).astype(jnp.bfloat16)
    tall = 2 * planes + EXTRA
    weights[:tall] = high
    weights[tall:] = low
    for side, pick in ((0, at_column == 0), (1, at_column == last)):
        for part, values in ((0, real), (1, imag)):
            picked = jnp.sum(jnp.where(pick, values, 0.0), axis=1, keepdims=True)
            column[side, part] = jnp.broadcast_to(picked, (planes, 128))
    for part, values in ((0, real), (1, imag)):
        for side, pick in ((0, (at_row == last) & (at_column == 0)), (1, (at_row == 0) & (at_column == last))):
            picked = jnp.sum(jnp.sum(jnp.where(pick, values, 0.0), axis=1, keepdims=True), axis=0, keepdims=True)
            coeff[side, part] = jnp.broadcast_to(picked, (half, 128))

    def solve(s, r):
        load(s, r).wait()
        values = held[s, r].reshape(2 * planes, width)
        upper = values.astype(jnp.bfloat16)
        lower = (values - upper.astype(jnp.float32)).astype(jnp.bfloat16)
        first = jnp.dot(weights[...], upper, preferred_element_type=jnp.float32)
        second = jnp.dot(weights[:tall], lower, preferred_element_type=jnp.float32)
        total = first[:tall] + first[tall:] + second
        solved[s, r] = total[: 2 * planes].reshape(2, planes, width)
        side = s // half
        for part in range(2):
            row = jnp.where(
                side == 0,
                total[2 * planes + part : 2 * planes + part + 1],
                total[2 * planes + 2 + part : 2 * planes + 3 + part],
            )
            base[side, part, r + 2, pl.ds(s % half, 1), :] = row

    cut = planes - RELAY

    def piece(k, to_next, stop=planes):
        s, a, count_rows, part, parts = PIECES[k]
        row, at = (rows - a - count_rows, 2 - a - count_rows) if to_next else (a, 2 + a)
        return pltpu.make_async_remote_copy(
            src_ref=solved.at[s, pl.ds(row, count_rows), pl.ds(part, parts), pl.ds(0, stop)],
            dst_ref=halo.at[s, pl.ds(at, count_rows), pl.ds(part, parts), pl.ds(0, stop)],
            send_sem=bulk_send.at[int(to_next), k],
            recv_sem=bulk_recv.at[int(to_next), k],
            device_id=(d, l + 1 if to_next else l - 1),
            device_id_type=MESH,
        )

    relays = (
        (0, 0, (at_pair == 3) | ((at_pair == 7) & has_next), -1),
        (0, 1, (at_pair == 2) | ((at_pair == 6) & (l + 2 < tiles)), jnp.where(at_pair == 6, 7, -1)),
        (0, 2, (at_pair == 1) | ((at_pair == 5) & (l > 5)), jnp.where(at_pair == 5, -5, 3)),
        (1, 0, (at_pair == 4) | ((at_pair == 0) & has_prev), 1),
        (1, 1, (at_pair == 5) | ((at_pair == 1) & (l > 1)), jnp.where(at_pair == 1, -7, 1)),
        (1, 2, (at_pair == 6) | ((at_pair == 2) & (l + 6 < tiles)), jnp.where(at_pair == 2, 5, -3)),
    )
    relay_by = {(way, stage): by for way, stage, _, by in relays}

    def relay(way, stage):
        if stage == 0:
            kept = solved.at[0, 0 if way else rows - 1, 0, pl.ds(cut, RELAY)]
        else:
            kept = passed.at[way, stage - 1]
        there = halo.at[0, 2 if way else 1, 0, pl.ds(cut, RELAY)] if stage == 2 else passed.at[way, stage]
        return pltpu.make_async_remote_copy(
            src_ref=kept,
            dst_ref=there,
            send_sem=relay_send.at[way, stage],
            recv_sem=relay_recv.at[way, stage],
            device_id=(d, l + relay_by[way, stage]),
            device_id_type=MESH,
        )

    def relay_on(stage):
        for way, at, here, _ in relays:
            if at == stage:

                @pl.when(here)
                def _():
                    if stage > 0:
                        relay(way, stage - 1).wait_recv()
                    relay(way, stage).start()

    def send_pieces(start, stop):
        for to_next, there in ((False, has_prev), (True, has_next)):

            @pl.when(there)
            def _():
                for k in range(start, stop):
                    piece(k, to_next).start()

    def send_first(to_next, there, stop):
        @pl.when(there)
        def _():
            piece(0, to_next, stop).start()
            for k in range(1, AFTER_FIRST):
                piece(k, to_next).start()

    solve(0, 0)
    solve(0, 3)

    def tell_layers():
        for there, by_d in ((has_above, -1), (has_below, 1)):

            @pl.when(there)
            def _():
                pl.semaphore_signal(ready_sem, inc=1, device_id=(d + by_d, l), device_id_type=MESH)

    @pl.when(jnp.logical_not(seam))
    def _():
        pl.semaphore_wait(barrier, tiles_beside + tiles_beyond + layers_beside)
        for there, by_l in ((has_prev & seam_at(l - 1), -1), (has_next & seam_at(l + 1), 1)):

            @pl.when(there)
            def _():
                pl.semaphore_signal(near_sem, inc=1, device_id=(d, l + by_l), device_id_type=MESH)

    @pl.when(seam)
    def _():
        pl.semaphore_wait(near_sem, 1)

    near_prev = has_prev & jnp.logical_not(seam_prev)
    near_next = has_next & jnp.logical_not(seam_next)
    send_first(False, near_prev, planes)
    send_first(True, near_next, planes)

    @pl.when(jnp.logical_not(seam))
    def _():
        tell_layers()

    @pl.when(seam)
    def _():
        pl.semaphore_wait(barrier, 1)

    send_first(False, seam_prev, cut)
    send_first(True, seam_next, cut)
    relay_on(0)
    solve(0, 1)
    solve(0, 2)
    send_pieces(AFTER_FIRST, AFTER_SHOT)

    def solve_shot(s, carry):
        for r in range(rows):
            solve(s, r)
        return carry

    lax.fori_loop(1, shots, solve_shot, 0)

    def base_copy(side, to_next):
        source_at, target_at = (4, 0) if to_next else (2, 6)
        return pltpu.make_async_remote_copy(
            src_ref=base.at[side, :, pl.ds(source_at, 2)],
            dst_ref=base.at[side, :, pl.ds(target_at, 2)],
            send_sem=base_send.at[int(to_next), side],
            recv_sem=base_recv.at[int(to_next), side],
            device_id=(d, l + 1 if to_next else l - 1),
            device_id_type=MESH,
        )

    base_copies = tuple(
        (needed, to_next, side)
        for needed, side in ((True, side_one), (inner, side_two))
        for to_next in (False, True)
    )

    def both(needed, there):
        return there if needed is True else needed & there

    @pl.when(jnp.logical_not(seam))
    def _():
        pl.semaphore_wait(ready_sem, layers_beside)

    for needed, to_next, side in base_copies:

        @pl.when(both(needed, has_next if to_next else has_prev))
        def _():
            base_copy(side, to_next).start()

    @pl.when(inner)
    def _():
        send_pieces(AFTER_SHOT, AFTER_BASE_INNER)

    @pl.when(jnp.logical_not(inner))
    def _():
        send_pieces(AFTER_SHOT, AFTER_BASE_OUTER)

    small[1].wait()
    small[2].wait()
    for r in range(rows):
        load_cells(r).wait()

        def look_up(i, carry):
            at = pl.ds(pl.multiple_of(i * BLOCK, BLOCK), BLOCK)
            kinds = cells[r, at, :]
            re = jnp.full(kinds.shape, table_re[0], jnp.float32)
            im = jnp.full(kinds.shape, table_im[0], jnp.float32)
            for kind in range(1, CLASSES):
                hit = kinds == kind
                re = jnp.where(hit, table_re[kind], re)
                im = jnp.where(hit, table_im[kind], im)
            kappa[r, 0, at, :] = re
            kappa[r, 1, at, :] = im
            bottom = lax.broadcasted_iota(jnp.int32, kinds.shape, 0) + i * BLOCK == last
            return (carry[0] + jnp.where(bottom, re, 0.0), carry[1] + jnp.where(bottom, im, 0.0))

        zeros = jnp.zeros((BLOCK, width), jnp.float32)
        sums = lax.fori_loop(0, planes // BLOCK, look_up, (zeros, zeros))
        for part in range(2):
            plane[0, part, r] = jnp.broadcast_to(jnp.sum(sums[part], axis=0, keepdims=True), (half, width))
            plane[1, part, r] = jnp.broadcast_to(kappa[r, part, pl.ds(0, 1), :], (half, width))

    for needed, to_next, side in base_copies:

        @pl.when(both(needed, has_prev if to_next else has_next))
        def _():
            base_copy(side, to_next).wait_recv()

    @pl.when(seam)
    def _():
        tell_layers()
        pl.semaphore_wait(ready_sem, layers_beside)

    relay_on(1)

    def lateral(values, r):
        at = r + 2
        return (
            NEAR * (values[at - 1] + values[at + 1])
            + FAR * (values[at - 2] + values[at + 2])
            + along_y(values[at])
            - 5.0 * values[at]
        )

    def trace_copies(side):
        to = d + 1 - 2 * side
        return (
            (
                True,
                True,
                lambda: pltpu.make_async_remote_copy(
                    src_ref=outbound.at[side],
                    dst_ref=inbound.at[side, :, pl.ds(2, 4)],
                    send_sem=trace_send.at[side, 0],
                    recv_sem=trace_recv.at[side, 0],
                    device_id=(to, l),
                    device_id_type=MESH,
                ),
            ),
            (
                has_prev,
                has_next,
                lambda: pltpu.make_async_remote_copy(
                    src_ref=outbound.at[side, :, pl.ds(0, 2)],
                    dst_ref=inbound.at[side, :, pl.ds(6, 2)],
                    send_sem=trace_send.at[side, 1],
                    recv_sem=trace_recv.at[side, 1],
                    device_id=(to, l - 1),
                    device_id_type=MESH,
                ),
            ),
            (
                has_next,
                has_prev,
                lambda: pltpu.make_async_remote_copy(
                    src_ref=outbound.at[side, :, pl.ds(2, 2)],
                    dst_ref=inbound.at[side, :, pl.ds(0, 2)],
                    send_sem=trace_send.at[side, 2],
                    recv_sem=trace_recv.at[side, 2],
                    device_id=(to, l + 1),
                    device_id_type=MESH,
                ),
            ),
        )

    def under(there, act):
        if there is True:
            act()
        else:
            pl.when(there)(act)

    def emit(side):
        factor = [
            jnp.concatenate([coeff[side, part]] * (width // 128), axis=1) for part in range(2)
        ]
        planar = ([], [])
        for row in range(rows + 4):
            t_re, t_im = inbound[side, 0, row], inbound[side, 1, row]
            planar[0].append(base[side, 0, row] + factor[0] * t_re - factor[1] * t_im)
            planar[1].append(base[side, 1, row] + factor[0] * t_im + factor[1] * t_re)
        for r in range(rows):
            re, im = planar[0][r + 2], planar[1][r + 2]
            k_re, k_im = plane[side, 0, r], plane[side, 1, r]
            outbound[side, 0, r] = re + CORRECTION * (lateral(planar[0], r) + k_re * re - k_im * im)
            outbound[side, 1, r] = im + CORRECTION * (lateral(planar[1], r) + k_re * im + k_im * re)
        for goes, _, copy in trace_copies(side):
            under(goes, lambda: copy().start())

    def take(side):
        for _, comes, copy in trace_copies(side):
            under(comes, lambda: copy().wait_recv())

    @pl.when(inner)
    def _():
        take(side_one)

    emit(side_one)

    @pl.when(inner)
    def _():
        send_pieces(AFTER_BASE_INNER, AFTER_TRACE_INNER)

    @pl.when(jnp.logical_not(inner))
    def _():
        send_pieces(AFTER_BASE_OUTER, AFTER_TRACE_OUTER)

    take(side_two)

    @pl.when(inner)
    def _():
        emit(side_two)

    relay_on(2)

    @pl.when(inner)
    def _():
        send_pieces(AFTER_TRACE_INNER, len(PIECES))

    @pl.when(jnp.logical_not(inner))
    def _():
        send_pieces(AFTER_TRACE_OUTER, len(PIECES))

    for side in range(2):
        for part in range(2):
            values = [inbound[side, part, row] for row in range(rows + 4)]
            for r in range(rows):
                spread[side, part, r] = values[r + 2] + CORRECTION * lateral(values, r)

    def own_rows(s, carry):
        side, shot = s // half, s % half
        for r in range(rows):
            t = [inbound[side, part, r + 2, pl.ds(shot, 1), :] for part in range(2)]
            e = [spread[side, part, r, pl.ds(shot, 1), :] for part in range(2)]

            def block(i, inside):
                at = pl.ds(pl.multiple_of(i * BLOCK, BLOCK), BLOCK)
                g_re, g_im = (
                    jnp.concatenate([column[side, part, at, :]] * (width // 128), axis=1) for part in range(2)
                )
                linear, values = [], []
                for part in range(2):
                    v = solved[s, r, part, at, :]
                    near = [solved[s, q, part, at, :] for q in (r - 1, r + 1) if 0 <= q < rows]
                    far = [solved[s, q, part, at, :] for q in (r - 2, r + 2) if 0 <= q < rows]
                    total = along_y(v) - 5.0 * v + NEAR * sum(near[1:], near[0]) + FAR * sum(far[1:], far[0])
                    linear.append(v + CORRECTION * total)
                    values.append(v)
                v_re = values[0] + g_re * t[0] - g_im * t[1]
                v_im = values[1] + g_re * t[1] + g_im * t[0]
                k_re, k_im = kappa[r, 0, at, :], kappa[r, 1, at, :]
                field[s, r, 0, at, :] = (
                    linear[0] + g_re * e[0] - g_im * e[1] + CORRECTION * (k_re * v_re - k_im * v_im)
                )
                field[s, r, 1, at, :] = (
                    linear[1] + g_re * e[1] + g_im * e[0] + CORRECTION * (k_re * v_im + k_im * v_re)
                )
                return inside

            lax.fori_loop(0, planes // BLOCK, block, 0)
        return carry

    lax.fori_loop(0, shots, own_rows, 0)

    def add_rows(s, part, q, to_rows, start=0, stop=planes):
        for first in range(start, stop, BLOCK):
            at = pl.ds(first, min(BLOCK, stop - first))
            v = halo[s, q, part, at, :]
            for r, weight in to_rows:
                field[s, r, part, at, :] = field[s, r, part, at, :] + (CORRECTION * weight) * v

    for needed, to_next, side in base_copies:

        @pl.when(both(needed, has_next if to_next else has_prev))
        def _():
            base_copy(side, to_next).wait_send()

    for goes, _, copy in trace_copies(side_one):
        under(goes, lambda: copy().wait_send())

    @pl.when(inner)
    def _():
        for goes, _, copy in trace_copies(side_two):
            under(goes, lambda: copy().wait_send())

    from_next = (((3, NEAR), (2, FAR)), ((3, FAR),))
    from_prev = (((0, NEAR), (1, FAR)), ((0, FAR),))

    def add_piece(k, to_next, there, stop=planes):
        s, first_row, count_rows, first_part, parts = PIECES[k]

        @pl.when(there)
        def _():
            piece(k, not to_next, stop).wait_recv()
            piece(k, to_next, stop).wait_send()
            for a in range(first_row, first_row + count_rows):
                q, to_rows = (2 + a, from_next[a]) if to_next else (1 - a, from_prev[a])

                def add_part(part, carry):
                    add_rows(s, part, q, to_rows, 0, stop)
                    return carry

                if parts == 1:
                    add_part(first_part, 0)
                else:
                    lax.fori_loop(first_part, first_part + parts, add_part, 0)

    add_piece(0, True, near_next)
    add_piece(0, False, near_prev)
    add_piece(0, True, seam_next, cut)
    add_piece(0, False, seam_prev, cut)
    for k in range(1, AFTER_TRACE_INNER):
        add_piece(k, True, has_next)
        add_piece(k, False, has_prev)
    for way, stage, here, _ in relays:

        @pl.when(here)
        def _():
            relay(way, stage).wait_send()

    for to_next, there in ((True, seam_next), (False, seam_prev)):

        @pl.when(there)
        def _():
            relay(1 if to_next else 0, 2).wait_recv()
            add_rows(0, 0, 2 if to_next else 1, (from_next if to_next else from_prev)[0], cut, planes)

    for k in range(AFTER_TRACE_INNER, len(PIECES)):
        add_piece(k, True, has_next)
        add_piece(k, False, has_prev)


def write_kernel(field, out, sem):
    shots, rows = field.shape[:2]

    def copy(s, r):
        return pltpu.make_async_copy(field.at[s, r], out.at[s, :, :, r, :], sem.at[s, r])

    for s in range(shots):
        for r in range(rows):
            copy(s, r).start()
    for s in range(shots):
        for r in range(rows):
            copy(s, r).wait()


def on_device(source, line_inverse, plane_count, classes, table_re, table_im):
    shots, parts, planes, rows, width = source.shape
    half = shots // 2
    by_rows = (shots, rows, parts, planes, width)
    any_space = pl.BlockSpec(memory_space=pl.ANY)
    hbm = pl.BlockSpec(memory_space=pltpu.HBM)
    vmem = pl.BlockSpec(memory_space=pltpu.VMEM)
    tall = 2 * planes + EXTRA
    pieces = len(PIECES)
    dma = pltpu.SemaphoreType.DMA
    operands = (source, line_inverse, classes, table_re, table_im)
    field = pl.pallas_call(
        field_kernel,
        out_shape=jax.ShapeDtypeStruct(by_rows, jnp.float32),
        in_specs=[pl.BlockSpec(memory_space=pltpu.SMEM)] + [hbm] * len(operands),
        out_specs=vmem,
        scratch_shapes=[
            pltpu.VMEM((parts, planes, planes), jnp.float32),
            pltpu.SMEM((CLASSES,), jnp.float32),
            pltpu.SMEM((CLASSES,), jnp.float32),
            pltpu.VMEM(by_rows, jnp.float32),
            pltpu.VMEM((rows, planes, width), jnp.int32),
            pltpu.VMEM(by_rows, jnp.float32),
            pltpu.VMEM((shots, 4, parts, planes, width), jnp.float32),
            pltpu.VMEM((rows, parts, planes, width), jnp.float32),
            pltpu.VMEM((2, parts, rows, half, width), jnp.float32),
            pltpu.VMEM((2, parts, rows + 4, half, width), jnp.float32),
            pltpu.VMEM((2, parts, rows + 4, half, width), jnp.float32),
            pltpu.VMEM((2, parts, rows, half, width), jnp.float32),
            pltpu.VMEM((2, parts, rows, half, width), jnp.float32),
            pltpu.VMEM((2, parts, planes, 128), jnp.float32),
            pltpu.VMEM((2, parts, half, 128), jnp.float32),
            pltpu.VMEM((2 * tall, 2 * planes), jnp.bfloat16),
            dma((3,)),
            dma((shots, rows)),
            dma((rows,)),
            dma((2, pieces)),
            dma((2, pieces)),
            dma((2, 2)),
            dma((2, 2)),
            dma((2, 3)),
            dma((2, 3)),
            pltpu.SemaphoreType.REGULAR,
            pltpu.SemaphoreType.REGULAR,
            dma((2, 3)),
            dma((2, 3)),
            pltpu.VMEM((2, 2, RELAY, width), jnp.float32),
        ],
        compiler_params=pltpu.CompilerParams(
            collective_id=0, has_side_effects=True, vmem_limit_bytes=40 * 2**20
        ),
    )(plane_count, *(pltpu.with_memory_space_constraint(x, pltpu.HBM) for x in operands))
    return pl.pallas_call(
        write_kernel,
        out_shape=jax.ShapeDtypeStruct(source.shape, jnp.float32),
        in_specs=[vmem],
        out_specs=any_space,
        scratch_shapes=[dma((shots, rows))],
        compiler_params=pltpu.CompilerParams(vmem_limit_bytes=8 * 2**20),
    )(field)


def solution(mesh):
    in_specs = (
        P(None, None, "depth", "lat", None),
        P("depth", None, None, None),
        P("depth"),
        P("depth", "lat", None),
        P(),
        P(),
    )
    out_specs = P(None, None, "depth", "lat", None)
    return jax.shard_map(
        on_device, mesh=mesh, in_specs=in_specs, out_specs=out_specs, check_vma=False
    )
```
